128 devices in a mesh: gx: 16 (over y_hi, z, core), gy: 8 (over y_lo, x).
Axes of the slice: x: 4, y: 4 (y_hi: 2, y_lo: 2; y = y_hi * 2 + y_lo), z: 4, core: 2. Of those that a mesh axis runs over, the one named last changes fastest.
Arguments:
- terminal: float32 [4096, 4096], P('gx', 'gy'), may hold values from -6 to 6
- crowding: float32 [4096, 4096], P('gx', 'gy'), may hold values from 0.5 to 4
- density: float32 [4096, 4096], P('gx', 'gy'), may hold values from 0.25 to 36, as said below
- fractions: float32 [4, 2, 4096, 4096], P(None, None, 'gx', 'gy'), may hold values from 0 to 1
- offsets: int32 [4, 8, 2], replicated, may hold values from -64 to 63
- control_cost: float32 [4, 8], replicated, may hold values from 0 to 4
Outputs:
- value_start: float32 [4096, 4096], P('gx', 'gy')
- density_end: float32 [4096, 4096], P('gx', 'gy')
- masses: float32 [4], replicated
The draws below stay inside these ranges and needn't reach their ends.
Inputs may be any that keep to these rules, and one draw needn't show every extreme that they name: `density`: positive.
All inputs are finite; a program needn't handle non-finite values.
Results may differ from the reference program's by a relative error of at most 0.0001.
Values sent between devices are 32-bit elements; how exact they have to be, the bound alone decides.
A program may use at most 128 MiB of HBM per device.

```python
import math
from functools import reduce
import jax
import jax.numpy as jnp
from jax import lax

STEPS = 4
CONTROLS = 8
REACH = 64
NX = 4096
NY = 4096


def draw_density(key, part):
    first = jax.random.fold_in(jax.random.fold_in(key, 7), 0)
    rough = jnp.exp(jax.random.uniform(first, (NX, NY), jnp.float32, jnp.log(0.25), jnp.log(4.0)))
    row_place = jnp.arange(NX, dtype=jnp.float32) / NX
    profile = 1.0 + 2.0 * row_place[:, None] + jnp.zeros((NX, NY), jnp.float32)
    return jnp.clip(rough * profile, 0.25, 36.0)


def place_ends(values, rng, low, top_value):
    longest = values.shape.index(max(values.shape))
    spots = []
    for shift in (0, 1):
        where = [jax.random.randint(jax.random.fold_in(rng, axis), (), 0, length) for axis, length in enumerate(values.shape)]
        where[longest] = (where[longest] + shift) % values.shape[longest]
        spots.append(tuple(where))
    return values.at[spots[0]].set(low).at[spots[1]].set(top_value)


def steps_of(stream_key, dims, pieces, least, high):
    def one(position, blocks):
        heights = jax.random.uniform(jax.random.fold_in(jax.random.fold_in(stream_key, 6), position), (blocks,), jnp.float32, least / len(pieces), high / len(pieces))
        return jnp.repeat(jnp.exp(heights), dims[position] // blocks).reshape((-1,) + (1,) * (len(dims) - position - 1))

    level = one(*pieces[0])
    for cut in pieces[1:]:
        level = level * one(*cut)
    return level


def noise(stream_key, shape, spread, bound, cuts=(), kind=jnp.bfloat16):
    entries = jax.random.normal(stream_key, shape, jnp.float32) * spread
    if len(cuts) > 0:
        entries = steps_of(stream_key, shape, cuts, -0.22, 0.18) * entries
    return jnp.clip(entries, min=-bound, max=bound).astype(kind)


def setup_inputs(seed: int = 0) -> dict:
    arg_keys = jax.random.split(jax.random.key(seed), 7)
    terminal = noise(arg_keys[0], (NX, NY), 1.0, 6.0, ((0, 16), (1, 8)), jnp.float32)
    crowding = jnp.clip(jnp.exp(math.log(4.0) - 2.0794415 * jax.random.uniform(arg_keys[1], (NX, NY), jnp.float32) ** steps_of(arg_keys[1], (NX, NY), ((0, 16), (1, 8)), -0.2, 0.2)), 0.5, 4.0)
    density = draw_density(jax.random.fold_in(arg_keys[6], 71), 0)
    fractions = jnp.clip(1.0 * jax.random.uniform(arg_keys[3], (STEPS, 2, NX, NY), jnp.float32) ** steps_of(arg_keys[3], (STEPS, 2, NX, NY), ((2, 16), (3, 8)), -0.2, 0.2), 0.0, 1.0)
    offsets = place_ends(jax.random.randint(arg_keys[4], (STEPS, CONTROLS, 2), -REACH, REACH), jax.random.fold_in(arg_keys[4], 1), -REACH, REACH - 1).astype(jnp.int32)
    control_cost = jnp.clip(jax.random.uniform(arg_keys[5], (STEPS, CONTROLS), jnp.float32, 0.0, 4.0), 0.0, 4.0)
    return dict(terminal=terminal, crowding=crowding, density=density, fractions=fractions, offsets=offsets, control_cost=control_cost)


time_step = 0.1
temper = 0.3
epsilon = 1e-6


def catmull(fraction):
    square = fraction * fraction
    cube = square * fraction
    return [(-cube + 2.0 * square - fraction) * 0.5, (3.0 * cube - 5.0 * square + 2.0) * 0.5, (-3.0 * cube + 4.0 * square + fraction) * 0.5, (cube - square) * 0.5]


def sample(padded, weights_x, weights_y, shift_row, shift_col, margin, height, breadth):
    summed = None
    for row_tap in range(4):
        partial_sum = None
        for col_tap in range(4):
            piece = lax.dynamic_slice(padded, (margin + shift_row + row_tap - 1, margin + shift_col + col_tap - 1), (height, breadth))
            term = weights_y[col_tap] * piece
            partial_sum = term if partial_sum is None else partial_sum + term
        term = weights_x[row_tap] * partial_sum
        summed = term if summed is None else summed + term
    return summed


def option_values(padded, weights_x, weights_y, offsets, control_cost, crowding, moment, margin, height, breadth):
    candidates = []
    for option in range(offsets.shape[1]):
        shifted = sample(padded, weights_x, weights_y, offsets[moment, option, 0], offsets[moment, option, 1], margin, height, breadth)
        candidates.append(shifted + time_step * (control_cost[moment, option] + crowding))
    return candidates


def policy(candidates):
    lowest = reduce(jnp.minimum, candidates)
    ramps = [jnp.maximum(lowest + temper - candidate, 0.0) for candidate in candidates]
    ramp_sum = reduce(jnp.add, ramps)
    return lowest, [ramp / ramp_sum for ramp in ramps]


def reference(terminal, crowding, density, fractions, offsets, control_cost):
    margin = REACH + 2
    height, breadth = terminal.shape
    current_value = terminal
    policies = [None] * STEPS
    for moment in reversed(range(STEPS)):
        padded = jnp.pad(current_value, margin, mode="wrap")
        weights_x = catmull(fractions[moment, 0])
        weights_y = catmull(fractions[moment, 1])
        candidates = option_values(padded, weights_x, weights_y, offsets, control_cost, crowding, moment, margin, height, breadth)
        current_value, policies[moment] = policy(candidates)
    current = density
    mass_list = []
    for moment in range(STEPS):
        weights_x = catmull(fractions[moment, 0])
        weights_y = catmull(fractions[moment, 1])
        padded = jnp.pad(current, margin, mode="wrap")
        arrived = None
        for option in range(CONTROLS):
            shifted = sample(padded, weights_x, weights_y, -offsets[moment, option, 0], -offsets[moment, option, 1], margin, height, breadth)
            term = policies[moment][option] * shifted
            arrived = term if arrived is None else arrived + term
        arrived = jnp.maximum(arrived, 0.0)
        mean_mass = jnp.sum(arrived) / (NX * NY)
        mass_list.append(mean_mass)
        current = arrived / (mean_mass + epsilon)
    return current_value, current, jnp.stack(mass_list)
```

```python
import functools

import jax
import jax.numpy as jnp
from jax import lax
from jax.experimental import pallas as pl
from jax.experimental.pallas import tpu as pltpu
from jax.sharding import PartitionSpec as P

MESH = pl.DeviceIdType.MESH
LANES = 128
HALO = 72
CHUNK = 64
GROWS = CHUNK + 8
PIECE = 24

time_step = 0.1
temper = 0.3
epsilon = 1e-06


def catmull(t):
    square = t * t
    last = (0.5 * t) * (square - t)
    first = 0.5 * (square - t) - last
    third = 0.5 * (square + t) - 3.0 * last
    second = 1.0 - first - third - last
    return [first, second, third, last]


def kernel(
    off, cost, term, crowd, dens, frac,
    value_out, mass_out, sums,
    ea, eb, ec, ga, gb, wts, ramps, recip, cr, fr,
    load_sem, send_sem, recv_sem,
):
    rows, cols = term.shape
    tiles = cols // LANES
    steps, controls = cost.shape
    chunks = rows // CHUNK
    nx, ny = lax.axis_size("gx"), lax.axis_size("gy")
    x, y = lax.axis_index("gx"), lax.axis_index("gy")
    up, down = lax.rem(x + nx - 1, nx), lax.rem(x + 1, nx)
    left, right = lax.rem(y + ny - 1, ny), lax.rem(y + 1, ny)
    lane = lax.broadcasted_iota(jnp.int32, (PIECE, LANES), 1)

    barrier = pltpu.get_barrier_semaphore()
    around = [(i, j) for i in (up, x, down) for j in (left, y, right)]
    around.pop(4)
    for i, j in around:
        pl.semaphore_signal(barrier, inc=1, device_id=(i, j), device_id_type=MESH)

    def load_field(src, buf, first):
        return [
            pltpu.make_async_copy(
                src.at[:, pl.ds(c * LANES, LANES)],
                buf.at[1 + c, pl.ds(HALO, rows), :],
                load_sem.at[first + c],
            )
            for c in range(tiles)
        ]

    load_term = load_field(term, ea, 0)
    load_dens = load_field(dens, ec, tiles)
    load_cr = pltpu.make_async_copy(crowd, cr, load_sem.at[2 * tiles])
    load_fr = [
        pltpu.make_async_copy(frac.at[n], fr.at[n], load_sem.at[2 * tiles + 1 + n])
        for n in range(steps)
    ]
    for copy in load_term:
        copy.start()
    load_fr[steps - 1].start()
    load_cr.start()
    for copy in load_fr[: steps - 1]:
        copy.start()
    for copy in load_dens:
        copy.start()

    low, high = HALO, HALO + rows
    mid = pl.ds(1, tiles)

    def exchange(buf, slot):
        def send(index, src_tile, src_row, dst_tile, dst_row, count, i, j):
            return pltpu.make_async_remote_copy(
                src_ref=buf.at[src_tile, pl.ds(src_row, count), :],
                dst_ref=buf.at[dst_tile, pl.ds(dst_row, count), :],
                send_sem=send_sem.at[slot, index],
                recv_sem=recv_sem.at[slot, index],
                device_id=(i, j),
                device_id_type=MESH,
            )

        one, many, end = pl.ds(1, 1), pl.ds(tiles, 1), pl.ds(tiles + 1, 1)
        zero = pl.ds(0, 1)
        north = [
            send(0, mid, low, mid, high, HALO, up, y),
            send(2, one, low, end, high, HALO, up, left),
            send(3, many, low, zero, high, HALO, up, right),
        ]
        south = [
            send(1, mid, high - HALO, mid, 0, HALO, down, y),
            send(4, one, high - HALO, end, 0, HALO, down, left),
            send(5, many, high - HALO, zero, 0, HALO, down, right),
        ]
        sides = []
        for q in range(chunks):
            r = low + q * CHUNK
            sides.append(
                [
                    send(6 + q, one, r, end, r, CHUNK, x, left),
                    send(6 + chunks + q, many, r, zero, r, CHUNK, x, right),
                ]
            )
        return north, south, sides

    def every(buf, slot):
        north, south, sides = exchange(buf, slot)
        return north + south + [d for pair in sides for d in pair]

    def weights_pass(n):
        def body(i, _):
            r = pl.ds(pl.multiple_of(i * 8, 8), 8)
            for c in range(tiles):
                lanes = pl.ds(c * LANES, LANES)
                wx = catmull(fr[n, 0, r, lanes])
                wy = catmull(fr[n, 1, r, lanes])
                for a in range(4):
                    for b in range(4):
                        wts[a * 4 + b, c, r, :] = wx[a] * wy[b]
            return 0

        lax.fori_loop(0, rows // 8, body, 0)

    def shift(src, dst, n, k, row0, sign):
        a, b = sign * off[n, k, 0], sign * off[n, k, 1]
        start = HALO + row0 + a - 1
        for s in range(4):
            total = LANES + b + s - 1
            tile = lax.shift_right_logical(total, 7)
            by = lax.bitwise_and(total, LANES - 1)
            amount = lax.bitwise_and(LANES - by, LANES - 1)
            keep = lane < LANES - by
            for p in range(0, GROWS, PIECE):
                turned = [
                    pltpu.roll(src[tile + c, pl.ds(start + p, PIECE), :], amount, 1)
                    for c in range(tiles + 1)
                ]
                for c in range(tiles):
                    dst[k, s, c, p : p + PIECE, :] = jnp.where(keep, turned[c], turned[c + 1])

    def sample(src, w, k, c, j):
        acc = None
        for a in range(4):
            for b in range(4):
                part = w[a * 4 + b] * src[k, b, c, pl.ds(j + a, 8), :]
                acc = part if acc is None else acc + part
        return acc

    def backward_rows(src, dst, n, row0, i):
        j = pl.multiple_of(i * 8, 8)
        r = pl.ds(pl.multiple_of(row0 + j, 8), 8)
        for c in range(tiles):
            w = [wts[m, c, r, :] for m in range(16)]
            q = [sample(src, w, k, c, j) + time_step * cost[n, k] for k in range(controls)]
            lowest = functools.reduce(jnp.minimum, q)
            edge = lowest + temper
            total = None
            for k in range(controls):
                ramp = jnp.maximum(edge - q[k], 0.0)
                ramps[n * controls + k, c, r, :] = ramp
                total = ramp if total is None else total + ramp
            recip[n, c, r, :] = 1.0 / total
            here = pl.ds(pl.multiple_of(HALO + row0 + j, 8), 8)
            dst[1 + c, here, :] = lowest + time_step * cr[r, pl.ds(c * LANES, LANES)]

    def forward_rows(src, dst, n, row0, i):
        j = pl.multiple_of(i * 8, 8)
        r = pl.ds(pl.multiple_of(row0 + j, 8), 8)
        added = sums[n]
        for c in range(tiles):
            w = [wts[m, c, r, :] for m in range(16)]
            acc = None
            for k in range(controls):
                part = ramps[n * controls + k, c, r, :] * sample(src, w, k, c, j)
                acc = part if acc is None else acc + part
            acc = jnp.maximum(acc * recip[n, c, r, :], 0.0)
            here = pl.ds(pl.multiple_of(HALO + row0 + j, 8), 8)
            dst[1 + c, here, :] = acc
            added = added + acc
        sums[n] = added

    order = [0, chunks - 1] + list(range(1, chunks - 1))

    def stage(src, dst, slot_src, slot_dst, n, sign, rows_fn, send):
        weights_pass(n)
        for d in every(src, slot_src):
            d.wait()
        north, south, sides = exchange(dst, slot_dst)

        def first(k, _):
            shift(src, ga, n, k, order[0] * CHUNK, sign)
            return 0

        lax.fori_loop(0, controls, first, 0)
        now, later = ga, gb
        for at, q in enumerate(order):
            following = order[at + 1] if at + 1 < chunks else None

            def body(i, _):
                rows_fn(now, dst, n, q * CHUNK, i)
                if following is not None:
                    shift(src, later, n, i, following * CHUNK, sign)
                return 0

            lax.fori_loop(0, CHUNK // 8, body, 0)
            now, later = later, now
            todo = list(sides[q])
            if q == 1:
                todo += north
            if q == chunks - 2:
                todo += south

            def go():
                for d in todo:
                    d.start()

            if send is True:
                go()
            else:
                pl.when(send)(go)

    for copy in load_term:
        copy.wait()
    pl.semaphore_wait(barrier, 8)
    for d in every(ea, 0):
        d.start()
    for copy in load_dens:
        copy.wait()
    for d in every(ec, 2):
        d.start()
    load_fr[steps - 1].wait()
    load_cr.wait()
    for copy in load_fr[: steps - 1]:
        copy.wait()
    sums[...] = jnp.zeros_like(sums)

    def backward_pair(m, _):
        n = steps - 1 - 2 * m
        stage(ea, eb, 0, 1, n, 1, backward_rows, True)
        stage(eb, ea, 1, 0, n - 1, 1, backward_rows, m + 1 < steps // 2)
        return 0

    lax.fori_loop(0, steps // 2, backward_pair, 0)

    def store_field(buf, dst, first):
        return [
            pltpu.make_async_copy(
                buf.at[1 + c, pl.ds(HALO, rows), :],
                dst.at[:, pl.ds(c * LANES, LANES)],
                load_sem.at[first + c],
            )
            for c in range(tiles)
        ]

    for copy in store_field(ea, value_out, 0):
        copy.start()
    for copy in store_field(ea, value_out, 0):
        copy.wait()

    def forward_pair(m, _):
        n = 2 * m
        stage(ec, ea, 2, 0, n, -1, forward_rows, True)
        stage(ea, ec, 0, 2, n + 1, -1, forward_rows, m + 1 < steps // 2)
        return 0

    lax.fori_loop(0, steps // 2, forward_pair, 0)
    for copy in store_field(ec, mass_out, tiles):
        copy.start()
    for copy in store_field(ec, mass_out, tiles):
        copy.wait()


def shards(terminal, crowding, density, fractions, offsets, control_cost):
    rows, cols = terminal.shape
    tiles = cols // LANES
    steps, controls = control_cost.shape
    chunks = rows // CHUNK
    cells = rows * cols * lax.axis_size("gx") * lax.axis_size("gy")
    field = jax.ShapeDtypeStruct((rows, cols), jnp.float32)
    copies = 6 + 2 * chunks
    extended = pltpu.VMEM((tiles + 2, rows + 2 * HALO, LANES), jnp.float32)
    shifted = pltpu.VMEM((controls, 4, tiles, GROWS, LANES), jnp.float32)
    smem = pl.BlockSpec(memory_space=pltpu.SMEM)
    hbm = pl.BlockSpec(memory_space=pl.ANY)
    value, mass, sums = pl.pallas_call(
        kernel,
        out_shape=(field, field, jax.ShapeDtypeStruct((steps, 8, LANES), jnp.float32)),
        in_specs=[smem, smem, hbm, hbm, hbm, hbm],
        out_specs=(hbm, hbm, pl.BlockSpec(memory_space=pltpu.VMEM)),
        scratch_shapes=[
            extended, extended, extended, shifted, shifted,
            pltpu.VMEM((16, tiles, rows, LANES), jnp.float32),
            pltpu.VMEM((steps * controls, tiles, rows, LANES), jnp.float32),
            pltpu.VMEM((steps, tiles, rows, LANES), jnp.float32),
            pltpu.VMEM((rows, cols), jnp.float32),
            pltpu.VMEM((steps, 2, rows, cols), jnp.float32),
            pltpu.SemaphoreType.DMA((2 * tiles + 1 + steps,)),
            pltpu.SemaphoreType.DMA((3, copies)),
            pltpu.SemaphoreType.DMA((3, copies)),
        ],
        compiler_params=pltpu.CompilerParams(
            collective_id=0, has_side_effects=True, vmem_limit_bytes=60 * 2**20
        ),
    )(offsets, control_cost, terminal, crowding, density, fractions)
    totals = lax.psum(jnp.sum(sums, axis=(1, 2)), ("gx", "gy")) / cells
    masses, scale = [], jnp.float32(1.0)
    for n in range(steps):
        mean = totals[n] / scale
        masses.append(mean)
        scale = scale * (mean + epsilon)
    return value, mass / scale, jnp.stack(masses)


def solution(mesh):
    placed = (P("gx", "gy"), P("gx", "gy"), P("gx", "gy"), P(None, None, "gx", "gy"), P(), P())
    return jax.shard_map(
        shards,
        mesh=mesh,
        in_specs=placed,
        out_specs=(P("gx", "gy"), P("gx", "gy"), P()),
        check_vma=False,
    )
```

```python
import functools

import jax
import jax.numpy as jnp
from jax import lax
from jax.experimental import pallas as pl
from jax.experimental.pallas import tpu as pltpu
from jax.sharding import PartitionSpec as P

MESH = pl.DeviceIdType.MESH
LANES = 128
HALO = 72
PIECE = 24
BLOCK = 64
EDGE = 32

time_step = 0.1
temper = 0.3
epsilon = 1e-06


def catmull(t):
    square = t * t
    last = (0.5 * t) * (square - t)
    first = 0.5 * (square - t) - last
    third = 0.5 * (square + t) - 3.0 * last
    second = 1.0 - first - third - last
    return [first, second, third, last]


def kernel(
    off, cost, term, crowd, dens, frac,
    value_out, mass_out, masses_out,
    sums, part_y, part_x, ea, eb, ec, strips, packs, halo, moved,
    wts, ramps, recip, cr, fr, stage_a, stage_b, order,
    load_sem, send_sem, recv_sem, sum_send, sum_recv,
):
    rows, cols = term.shape
    tiles = cols // LANES
    taps = tiles + 3
    groups = rows // 8
    steps, controls = cost.shape
    nx, ny = lax.axis_size("gx"), lax.axis_size("gy")
    x, y = lax.axis_index("gx"), lax.axis_index("gy")
    up, down = lax.rem(x + nx - 1, nx), lax.rem(x + 1, nx)
    left, right = lax.rem(y + ny - 1, ny), lax.rem(y + 1, ny)
    low, high = HALO, HALO + rows

    def lanes_of(count):
        return lax.broadcasted_iota(jnp.int32, (count, LANES), 1)

    load_term = pltpu.make_async_copy(term, stage_a, load_sem.at[0])
    load_dens = pltpu.make_async_copy(dens, stage_b, load_sem.at[1])
    load_cr = pltpu.make_async_copy(crowd, cr, load_sem.at[2])
    load_fr = [
        pltpu.make_async_copy(frac.at[n], fr.at[n], load_sem.at[3 + n]) for n in range(steps)
    ]
    load_term.start()
    load_fr[steps - 1].start()
    load_cr.start()
    load_dens.start()
    for copy in load_fr[: steps - 1]:
        copy.start()

    barrier = pltpu.get_barrier_semaphore()
    around = [(i, j) for i in (up, x, down) for j in (left, y, right)]
    around.pop(4)
    for i, j in around:
        pl.semaphore_signal(barrier, inc=1, device_id=(i, j), device_id_type=MESH)

    def order_rows(i, _):
        here = pl.multiple_of(i * BLOCK, BLOCK)
        source = lax.broadcasted_iota(jnp.int32, (BLOCK, cols), 0) + here
        place = lax.broadcasted_iota(jnp.int32, (BLOCK, cols), 1)
        wanted = tiles * lax.bitwise_and(place, LANES - 1) + lax.shift_right_logical(place, 7)
        order[pl.ds(here, BLOCK), :] = jnp.where(source == wanted, 1.0, 0.0).astype(jnp.bfloat16)
        return 0

    lax.fori_loop(0, cols // BLOCK, order_rows, 0)

    def reorder(value, back):
        out = None
        rest = value
        for part in range(3):
            piece = rest.astype(jnp.bfloat16)
            if part < 2:
                rest = rest - piece.astype(jnp.float32)
            got = lax.dot_general(
                piece, order[...], (((1,), (1 if back else 0,)), ((), ())),
                preferred_element_type=jnp.float32,
            )
            out = got if out is None else out + got
        return out

    def each_block(body):
        def step(i, _):
            body(pl.multiple_of(i * BLOCK, BLOCK))
            return 0

        lax.fori_loop(0, rows // BLOCK, step, 0)

    def enter(src, buf):
        def body(r):
            got = reorder(src[pl.ds(r, BLOCK), :], False)
            here = pl.ds(pl.multiple_of(HALO + r, 8), BLOCK)
            for c in range(tiles):
                buf[c, here, :] = got[:, c * LANES : (c + 1) * LANES]

        each_block(body)

    def leave(buf, dst, factor):
        def body(r):
            here = pl.ds(pl.multiple_of(HALO + r, 8), BLOCK)
            whole = jnp.concatenate([buf[c, here, :] for c in range(tiles)], axis=1)
            if factor is not None:
                whole = whole * factor
            dst[pl.ds(r, BLOCK), :] = reorder(whole, True)

        each_block(body)

    def in_place(ref):
        def body(r):
            ref[pl.ds(r, BLOCK), :] = reorder(ref[pl.ds(r, BLOCK), :], False)

        each_block(body)

    def pack(buf, slot, first, count):
        lane = lanes_of(8 * count)
        here = slice(HALO + 8 * first, HALO + 8 * (first + count))
        there = slice(8 * first, 8 * (first + count))
        tile = [buf[c, here, :] for c in range(tiles)]
        for side in range(2):
            out = None
            for c in range(tiles):
                by = EDGE * (c + side) % LANES
                turned = pltpu.roll(tile[c], by, 1) if by else tile[c]
                out = turned if out is None else jnp.where(lane < EDGE * c, out, turned)
            packs[slot, side, there, :] = out

    def unpack(slot):
        def body(i, _):
            r = pl.ds(pl.multiple_of(i * 40, 8), 40)
            lane = lanes_of(40)
            near, far = strips[slot, 0, r, :], strips[slot, 1, r, :]
            for c in range(tiles):
                by, bx = (LANES - EDGE * c) % LANES, EDGE * (tiles - 1 - c)
                a = pltpu.roll(near, by, 1) if by else near
                b = pltpu.roll(far, bx, 1) if bx else far
                halo[c, r, :] = jnp.where(lane < LANES // 2, a, b)
            return 0

        lax.fori_loop(0, (rows + 2 * HALO) // 40, body, 0)

    def exchange(buf, slot):
        def send(index, src, dst, i, j):
            return pltpu.make_async_remote_copy(
                src_ref=src,
                dst_ref=dst,
                send_sem=send_sem.at[slot, index],
                recv_sem=recv_sem.at[slot, index],
                device_id=(i, j),
                device_id_type=MESH,
            )

        def side(index, which, src_row, dst_row, count, i, j):
            return send(
                index,
                packs.at[slot, which, pl.ds(src_row, count), :],
                strips.at[slot, which, pl.ds(dst_row, count), :],
                i, j,
            )

        last = rows - HALO
        outer = [
            send(0, buf.at[:, pl.ds(low, HALO), :], buf.at[:, pl.ds(high, HALO), :], up, y),
            send(1, buf.at[:, pl.ds(high - HALO, HALO), :], buf.at[:, pl.ds(0, HALO), :], down, y),
            side(2, 0, 0, low, HALO, x, left),
            side(3, 1, 0, low, HALO, x, right),
            side(4, 0, last, low + last, HALO, x, left),
            side(5, 1, last, low + last, HALO, x, right),
            side(6, 0, 0, high, HALO, up, left),
            side(7, 1, 0, high, HALO, up, right),
            side(8, 0, last, 0, HALO, down, left),
            side(9, 1, last, 0, HALO, down, right),
        ]
        inner = [
            side(10, 0, HALO, low + HALO, rows - 2 * HALO, x, left),
            side(11, 1, HALO, low + HALO, rows - 2 * HALO, x, right),
        ]
        return outer, inner

    rim, core = HALO // 8, (rows - 2 * HALO) // 8

    def pack_outer(buf, slot):
        pack(buf, slot, 0, rim)
        pack(buf, slot, groups - rim, rim)

    def pack_inner(buf, slot):
        half = core // 2
        pack(buf, slot, rim, half)
        pack(buf, slot, rim + half, core - half)

    def weights_pass(n):
        def body(i, _):
            r = pl.ds(pl.multiple_of(i * 8, 8), 8)
            for c in range(tiles):
                lanes = pl.ds(c * LANES, LANES)
                wx = catmull(fr[n, 0, r, lanes])
                wy = catmull(fr[n, 1, r, lanes])
                for a in range(4):
                    for b in range(4):
                        wts[c, i, a * 4 + b] = wx[a] * wy[b]
            return 0

        lax.fori_loop(0, groups, body, 0)

    def shift(src, n, k, sign):
        a, b = sign * off[n, k, 0], sign * off[n, k, 1]
        start = HALO + a - 1
        lane = lanes_of(PIECE)
        for m in range(taps):
            total = b + (m - 1)
            tile = lax.bitwise_and(total, tiles - 1)
            by = lax.shift_right_arithmetic(total, tiles.bit_length() - 1)
            amount = lax.bitwise_and(-by, LANES - 1)
            inside = lane - by
            mine = jnp.logical_and(inside >= 0, inside < LANES)
            for p in range(0, rows + 8, PIECE):
                r = pl.ds(start + p, PIECE)
                both = jnp.where(mine, src[tile, r, :], halo[tile, r, :])
                moved[k, m, p : p + PIECE, :] = pltpu.roll(both, amount, 1)

    def sample(w, k, c, j):
        acc = None
        for a in range(4):
            for b in range(4):
                part = w[a * 4 + b] * moved[k, c + b, pl.ds(j + a, 8), :]
                acc = part if acc is None else acc + part
        return acc

    def backward_rows(dst, n, g):
        j = pl.multiple_of(g * 8, 8)
        here = pl.ds(pl.multiple_of(HALO + j, 8), 8)
        for c in range(tiles):
            w = [wts[c, g, m] for m in range(16)]
            q = [sample(w, k, c, j) + time_step * cost[n, k] for k in range(controls)]
            lowest = functools.reduce(jnp.minimum, q)
            edge = lowest + temper
            total = None
            for k in range(controls):
                ramp = jnp.maximum(edge - q[k], 0.0)
                ramps[n, c, g, k] = ramp
                total = ramp if total is None else total + ramp
            recip[n, c, g] = 1.0 / total
            dst[c, here, :] = lowest + time_step * cr[pl.ds(j, 8), pl.ds(c * LANES, LANES)]

    def forward_rows(dst, n, g):
        j = pl.multiple_of(g * 8, 8)
        here = pl.ds(pl.multiple_of(HALO + j, 8), 8)
        added = sums[n]
        for c in range(tiles):
            w = [wts[c, g, m] for m in range(16)]
            acc = None
            for k in range(controls):
                part = ramps[n, c, g, k] * sample(w, k, c, j)
                acc = part if acc is None else acc + part
            acc = jnp.maximum(acc * recip[n, c, g], 0.0)
            dst[c, here, :] = acc
            added = added + acc
        sums[n] = added

    def wait_all(buf, slot):
        outer, inner = exchange(buf, slot)
        for d in outer + inner:
            d.wait()

    def stage(src, dst, slot_src, slot_dst, n, sign, rows_fn, send, fresh):
        if fresh:
            in_place(fr.at[n, 0])
            in_place(fr.at[n, 1])
        weights_pass(n)
        wait_all(src, slot_src)
        unpack(slot_src)

        def shifts(k, _):
            shift(src, n, k, sign)
            return 0

        lax.fori_loop(0, controls, shifts, 0)
        outer, inner = exchange(dst, slot_dst)

        def publish(pack_fn, copies):
            def go():
                pack_fn(dst, slot_dst)
                for d in copies:
                    d.start()

            if send is True:
                go()
            else:
                pl.when(send)(go)

        def outer_rows(t, _):
            rows_fn(dst, n, t + core * (t // rim))
            return 0

        def inner_rows(t, _):
            rows_fn(dst, n, t + rim)
            return 0

        lax.fori_loop(0, 2 * rim, outer_rows, 0)
        publish(pack_outer, outer)
        lax.fori_loop(0, core, inner_rows, 0)
        publish(pack_inner, inner)

    def begin(load, src, buf, slot):
        load.wait()
        enter(src, buf)
        pack_outer(buf, slot)
        pack_inner(buf, slot)
        return [d for part in exchange(buf, slot) for d in part]

    first = begin(load_term, stage_a, ea, 0)
    pl.semaphore_wait(barrier, 8)
    for d in first:
        d.start()
    for d in begin(load_dens, stage_b, ec, 2):
        d.start()
    load_cr.wait()
    in_place(cr)
    for copy in load_fr:
        copy.wait()
    sums[...] = jnp.zeros_like(sums)

    def backward_pair(m, _):
        n = steps - 1 - 2 * m
        stage(ea, eb, 0, 1, n, 1, backward_rows, True, True)
        stage(eb, ea, 1, 0, n - 1, 1, backward_rows, m + 1 < steps // 2, True)
        return 0

    lax.fori_loop(0, steps // 2, backward_pair, 0)
    leave(ea, stage_a, None)
    store_value = pltpu.make_async_copy(stage_a, value_out, load_sem.at[0])
    store_value.start()

    def forward_pair(m, _):
        n = 2 * m
        stage(ec, ea, 2, 0, n, -1, forward_rows, True, False)
        stage(ea, ec, 0, 2, n + 1, -1, forward_rows, m + 1 < steps // 2, False)
        return 0

    lax.fori_loop(0, steps // 2, forward_pair, 0)

    def spread(part, count, at, own, first):
        copies = []
        for hop in range(1, count):
            copies.append(
                pltpu.make_async_remote_copy(
                    src_ref=part.at[0],
                    dst_ref=part.at[hop],
                    send_sem=sum_send.at[first + hop],
                    recv_sem=sum_recv.at[first + hop],
                    device_id=at(lax.rem(own + hop, count)),
                    device_id_type=MESH,
                )
            )
        for copy in copies:
            copy.start()
        for copy in copies:
            copy.wait()
        total = part[0]
        for hop in range(1, count):
            total = total + part[hop]
        return total

    own = [jnp.sum(sums[n], axis=0, keepdims=True) for n in range(steps)]
    part_y[0] = jnp.concatenate(own + [jnp.zeros((8 - steps, LANES), jnp.float32)], axis=0)
    part_x[0] = spread(part_y, ny, lambda j: (x, j), y, 0)
    whole = spread(part_x, nx, lambda i: (i, y), x, ny)
    totals = jnp.sum(whole, axis=1, keepdims=True) * (1.0 / (rows * cols * nx * ny))
    scale = jnp.ones((1, 1), jnp.float32)
    found = []
    for n in range(steps):
        mean = totals[n : n + 1, :] / scale
        found.append(mean)
        scale = scale * (mean + epsilon)
    found.append(jnp.zeros((8 - steps, 1), jnp.float32))
    masses_out[...] = jnp.broadcast_to(jnp.concatenate(found, axis=0), (8, LANES))
    factor = jnp.broadcast_to(1.0 / scale, (BLOCK, cols))

    leave(ec, stage_b, factor)
    store_mass = pltpu.make_async_copy(stage_b, mass_out, load_sem.at[1])
    store_mass.start()
    store_mass.wait()
    store_value.wait()


def shards(terminal, crowding, density, fractions, offsets, control_cost):
    rows, cols = terminal.shape
    tiles = cols // LANES
    steps, controls = control_cost.shape
    nx, ny = lax.axis_size("gx"), lax.axis_size("gy")
    field = jax.ShapeDtypeStruct((rows, cols), jnp.float32)
    tall = rows + 2 * HALO
    copies = 12

    def vmem(*shape):
        return pltpu.VMEM(shape, jnp.float32)

    smem = pl.BlockSpec(memory_space=pltpu.SMEM)
    hbm = pl.BlockSpec(memory_space=pl.ANY)
    value, mass, masses = pl.pallas_call(
        kernel,
        out_shape=(field, field, jax.ShapeDtypeStruct((8, LANES), jnp.float32)),
        in_specs=[smem, smem, hbm, hbm, hbm, hbm],
        out_specs=(hbm, hbm, pl.BlockSpec(memory_space=pltpu.VMEM)),
        scratch_shapes=[
            vmem(steps, 8, LANES),
            vmem(ny, 8, LANES),
            vmem(nx, 8, LANES),
            vmem(tiles, tall, LANES),
            vmem(tiles, tall, LANES),
            vmem(tiles, tall, LANES),
            vmem(3, 2, tall, LANES),
            vmem(3, 2, rows, LANES),
            vmem(tiles, tall, LANES),
            vmem(controls, tiles + 3, rows + 8, LANES),
            vmem(tiles, rows // 8, 16, 8, LANES),
            vmem(steps, tiles, rows // 8, controls, 8, LANES),
            vmem(steps, tiles, rows // 8, 8, LANES),
            vmem(rows, cols),
            vmem(steps, 2, rows, cols),
            vmem(rows, cols),
            vmem(rows, cols),
            pltpu.VMEM((cols, cols), jnp.bfloat16),
            pltpu.SemaphoreType.DMA((3 + steps,)),
            pltpu.SemaphoreType.DMA((3, copies)),
            pltpu.SemaphoreType.DMA((3, copies)),
            pltpu.SemaphoreType.DMA((nx + ny,)),
            pltpu.SemaphoreType.DMA((nx + ny,)),
        ],
        compiler_params=pltpu.CompilerParams(
            collective_id=0, has_side_effects=True, vmem_limit_bytes=60 * 2**20
        ),
    )(offsets, control_cost, terminal, crowding, density, fractions)
    return value, mass, masses[:steps, 0]


def solution(mesh):
    placed = (P("gx", "gy"), P("gx", "gy"), P("gx", "gy"), P(None, None, "gx", "gy"), P(), P())
    return jax.shard_map(
        shards,
        mesh=mesh,
        in_specs=placed,
        out_specs=(P("gx", "gy"), P("gx", "gy"), P()),
        check_vma=False,
    )
```

```python
import functools

import jax
import jax.numpy as jnp
from jax import lax
from jax.experimental import pallas as pl
from jax.experimental.pallas import tpu as pltpu
from jax.sharding import PartitionSpec as P

MESH = pl.DeviceIdType.MESH
LANES = 128
HALO = 72
PIECE = 24
BLOCK = 128
CHUNK = 64
GROWS = CHUNK + 8
EDGE = 32
LAG = 6
COPIES = 22

time_step = 0.1
temper = 0.3
epsilon = 1e-06


def catmull(t):
    square = t * t
    last = (0.5 * t) * (square - t)
    first = 0.5 * (square - t) - last
    third = 0.5 * (square + t) - 3.0 * last
    second = 1.0 - first - third - last
    return [first, second, third, last]


def kernel(
    off, cost, term, crowd, dens, frac,
    value_out, mass_out, masses_out,
    sums, part_y, part_x, ea, eb, ec, ends, strips, packs, ga, gb,
    wts, ramps, recip, cr, fr, stage_a, stage_b, order,
    load_sem, send_sem, recv_sem, sum_send, sum_recv,
):
    rows, cols = term.shape
    tiles = cols // LANES
    taps = tiles + 3
    groups = rows // 8
    steps, controls = cost.shape
    nx, ny = lax.axis_size("gx"), lax.axis_size("gy")
    x, y = lax.axis_index("gx"), lax.axis_index("gy")
    up, down = lax.rem(x + nx - 1, nx), lax.rem(x + 1, nx)
    left, right = lax.rem(y + ny - 1, ny), lax.rem(y + 1, ny)
    low, high = HALO, HALO + rows

    def lanes_of(count):
        return lax.broadcasted_iota(jnp.int32, (count, LANES), 1)

    load_term = pltpu.make_async_copy(term, stage_a, load_sem.at[0])
    load_dens = pltpu.make_async_copy(dens, stage_b, load_sem.at[1])
    load_cr = pltpu.make_async_copy(crowd, cr, load_sem.at[2])
    load_fr = [
        pltpu.make_async_copy(frac.at[n], fr.at[n], load_sem.at[3 + n]) for n in range(steps)
    ]
    load_term.start()
    load_fr[steps - 1].start()
    load_cr.start()
    load_dens.start()
    for copy in load_fr[: steps - 1]:
        copy.start()

    barrier = pltpu.get_barrier_semaphore()
    around = [(i, j) for i in (up, x, down) for j in (left, y, right)]
    around.pop(4)
    for i, j in around:
        pl.semaphore_signal(barrier, inc=1, device_id=(i, j), device_id_type=MESH)

    def order_rows(i, _):
        here = pl.multiple_of(i * BLOCK, BLOCK)
        source = lax.broadcasted_iota(jnp.int32, (BLOCK, cols), 0) + here
        place = lax.broadcasted_iota(jnp.int32, (BLOCK, cols), 1)
        wanted = tiles * lax.bitwise_and(place, LANES - 1) + lax.shift_right_logical(place, 7)
        order[pl.ds(here, BLOCK), :] = jnp.where(source == wanted, 1.0, 0.0).astype(jnp.bfloat16)
        return 0

    lax.fori_loop(0, cols // BLOCK, order_rows, 0)

    def reorder(value, back):
        count = value.shape[0]
        pieces = []
        rest = value
        for part in range(3):
            pieces.append(rest.astype(jnp.bfloat16))
            if part < 2:
                rest = rest - pieces[-1].astype(jnp.float32)
        got = lax.dot_general(
            jnp.concatenate(pieces, axis=0), order[...], (((1,), (1 if back else 0,)), ((), ())),
            preferred_element_type=jnp.float32,
        )
        return got[:count] + got[count : 2 * count] + got[2 * count :]

    def each_block(body):
        def step(i, _):
            body(pl.multiple_of(i * BLOCK, BLOCK))
            return 0

        lax.fori_loop(0, rows // BLOCK, step, 0)

    def enter(src, buf):
        def body(r):
            got = reorder(src[pl.ds(r, BLOCK), :], False)
            here = pl.ds(pl.multiple_of(HALO + r, 8), BLOCK)
            for c in range(tiles):
                buf[c, here, :] = got[:, c * LANES : (c + 1) * LANES]

        each_block(body)

    def leave(buf, dst, factor):
        def body(r):
            here = pl.ds(pl.multiple_of(HALO + r, 8), BLOCK)
            whole = jnp.concatenate([buf[c, here, :] for c in range(tiles)], axis=1)
            if factor is not None:
                whole = whole * factor
            dst[pl.ds(r, BLOCK), :] = reorder(whole, True)

        each_block(body)

    def in_place(ref):
        def body(r):
            ref[pl.ds(r, BLOCK), :] = reorder(ref[pl.ds(r, BLOCK), :], False)

        each_block(body)

    def pack(buf, slot, first, count):
        lane = lanes_of(8 * count)
        here = slice(HALO + 8 * first, HALO + 8 * (first + count))
        there = slice(8 * first, 8 * (first + count))
        tile = [buf[c, here, :] for c in range(tiles)]
        for side in range(2):
            out = None
            for c in range(tiles):
                by = EDGE * (c + side) % LANES
                turned = pltpu.roll(tile[c], by, 1) if by else tile[c]
                out = turned if out is None else jnp.where(lane < EDGE * c, out, turned)
            packs[slot, side, there, :] = out

    def unpack(buf, slot, first, last, turns):
        unit = 8 * (last - first) // turns

        def body(i, _):
            r = pl.ds(pl.multiple_of(first * 8 + i * unit, 8), unit)
            lane = lanes_of(unit)
            near, far = strips[slot, 0, r, :], strips[slot, 1, r, :]
            for c in range(tiles):
                by, bx = (LANES - EDGE * c) % LANES, EDGE * (tiles - 1 - c)
                a = pltpu.roll(near, by, 1) if by else near
                b = pltpu.roll(far, bx, 1) if bx else far
                buf[tiles + c, r, :] = jnp.where(lane < LANES // 2, a, b)
            return 0

        lax.fori_loop(0, turns, body, 0)

    def take_end(buf, slot, side):
        start = (0, high)[side]
        for c in range(tiles):
            buf[c, start : start + HALO, :] = ends[slot, side, c]

    def exchange(buf, slot):
        index = iter(range(COPIES))

        def send(src, dst, i, j):
            at = next(index)
            return pltpu.make_async_remote_copy(
                src_ref=src,
                dst_ref=dst,
                send_sem=send_sem.at[slot, at],
                recv_sem=recv_sem.at[slot, at],
                device_id=(i, j),
                device_id_type=MESH,
            )

        def rows_to(first, count, start, i):
            return [
                send(
                    packs.at[slot, which, pl.ds(first, count), :],
                    strips.at[slot, which, pl.ds(start, count), :],
                    i, j,
                )
                for which, j in ((0, left), (1, right))
            ]

        def north(first, count):
            return [
                send(
                    buf.at[pl.ds(0, tiles), pl.ds(low + first, count), :],
                    ends.at[slot, 1, :, pl.ds(first, count), :],
                    up, y,
                )
            ] + rows_to(first, count, high + first, up)

        def south(first, count):
            start = first - (rows - HALO)
            return [
                send(
                    buf.at[pl.ds(0, tiles), pl.ds(low + first, count), :],
                    ends.at[slot, 0, :, pl.ds(start, count), :],
                    down, y,
                )
            ] + rows_to(first, count, start, down)

        def side(first, count):
            return rows_to(first, count, low + first, x)

        rest = HALO - CHUNK
        end_d, side_d = south(rows - CHUNK, CHUNK), side(rows - CHUNK, CHUNK)
        end_a, side_a = north(0, CHUNK), side(0, CHUNK)
        side_c = side(2 * CHUNK - 8, CHUNK + 8)
        top_c = north(CHUNK, rest)
        late_c = side(CHUNK, 8) + south(rows - HALO, rest)
        side_b = side(HALO, CHUNK - 16)
        parts = {
            "d": end_d + side_d,
            "a": end_a + side_a,
            "c": side_c + top_c + late_c,
            "b": side_b,
        }
        early = end_a + top_c + side_d + side_c
        late = end_d + side_a + late_c + side_b
        return parts, early, late

    def weights_pass(n):
        def body(i, _):
            r = pl.ds(pl.multiple_of(i * 8, 8), 8)
            for c in range(tiles):
                lanes = pl.ds(c * LANES, LANES)
                wx = catmull(fr[n, 0, r, lanes])
                wy = catmull(fr[n, 1, r, lanes])
                for a in range(4):
                    for b in range(4):
                        wts[c, i, a * 4 + b] = wx[a] * wy[b]
            return 0

        lax.fori_loop(0, groups, body, 0)

    def shift(src, dst, n, k, row0, sign):
        a, b = sign * off[n, 0, k], sign * off[n, 1, k]
        start = HALO + row0 + a - 1
        lane = lanes_of(PIECE)
        held = {}

        def turn(m, p, first, second, split, amount):
            r = pl.ds(start + p, PIECE)
            both = jnp.where(lane < split, src[first, r, :], src[second, r, :])
            held[m, p] = pltpu.roll(both, amount, 1)

        def put(m, p):
            dst[k, m, p : p + PIECE, :] = held.pop((m, p))

        turns, puts = [], []
        for m in range(taps):
            total = b + (m - 1)
            tile = lax.bitwise_and(total, tiles - 1)
            by = lax.shift_right_arithmetic(total, tiles.bit_length() - 1)
            below = tiles * lax.shift_right_logical(by, 31)
            split = lax.bitwise_and(by, LANES - 1)
            amount = lax.bitwise_and(-by, LANES - 1)
            for p in range(0, GROWS, PIECE):
                turns.append(functools.partial(turn, m, p, tile + tiles - below, tile + below, split, amount))
                puts.append(functools.partial(put, m, p))
        return turns, puts

    def staggered(turns, puts, lag):
        for at in range(len(turns) + lag):
            now = []
            if at < len(turns):
                now.append(turns[at])
            if at >= lag:
                now.append(puts[at - lag])
            yield now

    def weave(main, side):
        done = 0
        for at, step in enumerate(main):
            step()
            due = (at + 1) * len(side) // len(main)
            for i in range(done, due):
                for one in side[i]:
                    one()
            done = due

    def sample(src, w, k, c, j):
        acc = None
        for a in range(4):
            for b in range(4):
                part = w[a * 4 + b] * src[k, c + b, pl.ds(j + a, 8), :]
                acc = part if acc is None else acc + part
        return acc

    def backward_rows(src, dst, n, row0, i):
        j = pl.multiple_of(i * 8, 8)
        g = row0 // 8 + i
        r = pl.ds(pl.multiple_of(row0 + j, 8), 8)
        here = pl.ds(pl.multiple_of(HALO + row0 + j, 8), 8)
        out = []
        for c in range(tiles):
            w, q = [], []

            def take(k, c=c, w=w, q=q):
                if k == 0:
                    w.extend(wts[c, g, m] for m in range(16))
                q.append(sample(src, w, k, c, j) + time_step * cost[n, k])
                if k == controls - 1:
                    lowest = functools.reduce(jnp.minimum, q)
                    edge = lowest + temper
                    total = None
                    for kk in range(controls):
                        ramp = jnp.maximum(edge - q[kk], 0.0)
                        ramps[n, c, g, kk] = ramp
                        total = ramp if total is None else total + ramp
                    recip[n, c, g] = 1.0 / total
                    dst[c, here, :] = lowest + time_step * cr[r, pl.ds(c * LANES, LANES)]

            out += [functools.partial(take, k) for k in range(controls)]
        return out

    def forward_rows(src, dst, n, row0, i):
        j = pl.multiple_of(i * 8, 8)
        g = row0 // 8 + i
        here = pl.ds(pl.multiple_of(HALO + row0 + j, 8), 8)
        out, added = [], []
        for c in range(tiles):
            w, acc = [], []

            def take(k, c=c, w=w, acc=acc):
                if k == 0:
                    w.extend(wts[c, g, m] for m in range(16))
                part = ramps[n, c, g, k] * sample(src, w, k, c, j)
                acc.append(part if k == 0 else acc[-1] + part)
                if k == controls - 1:
                    arrived = jnp.maximum(acc[-1] * recip[n, c, g], 0.0)
                    dst[c, here, :] = arrived
                    added.append(arrived)
                    if c == tiles - 1:
                        sums[n] = sums[n] + functools.reduce(jnp.add, added)

            out += [functools.partial(take, k) for k in range(controls)]
        return out

    per = CHUNK // 8
    mine = {"d": rows - CHUNK, "a": 0, "c": 2 * CHUNK, "b": CHUNK}

    def stage(src, dst, slot_src, slot_dst, n, sign, rows_fn, send, fresh):
        if fresh:
            in_place(fr.at[n, 0])
            in_place(fr.at[n, 1])
        weights_pass(n)
        _, early, late = exchange(src, slot_src)
        for d in early:
            d.wait()
        unpack(src, slot_src, 2 * (low // 8) + 6, (high + HALO) // 8, 2)
        take_end(src, slot_src, 1)

        def first(k, _):
            for now in staggered(*shift(src, ga, n, k, mine["d"], sign), 20):
                for one in now:
                    one()
            return 0

        lax.fori_loop(0, controls, first, 0)
        for d in late:
            d.wait()
        unpack(src, slot_src, 0, 2 * (low // 8) + 6, 3)
        take_end(src, slot_src, 0)
        parts, _, _ = exchange(dst, slot_dst)

        def publish(name, pieces):
            def go():
                for at, count in pieces:
                    pack(dst, slot_dst, at, count)
                for d in parts[name]:
                    d.start()

            if send is True:
                go()
            else:
                pl.when(send)(go)

        def block(now, later, name, following, start, stop, shift_from, place):
            def body(i, _):
                side = []
                if following is not None:
                    side = list(staggered(*shift(src, later, n, i + shift_from, mine[following], sign), LAG))
                weave(rows_fn(now, dst, n, mine[name], place(i)), side)
                return 0

            lax.fori_loop(start, stop, body, 0)

        def plain(i):
            return i

        block(ga, gb, "d", "a", 0, per, 0, plain)
        publish("d", [(mine["d"] // 8, per)])
        block(gb, ga, "a", "c", 0, per, 0, plain)
        publish("a", [(0, per)])
        block(ga, gb, "c", "b", 0, per, 0, plain)
        block(gb, None, "b", None, 0, 2, 0, lambda i: (per - 1) * (1 - i))
        publish("c", [(mine["c"] // 8 - 1, per + 1), (per, 1)])
        block(gb, None, "b", None, 1, per - 1, 0, plain)
        publish("b", [(per + 1, per - 2)])

    def begin(load, src, buf, slot):
        load.wait()
        enter(src, buf)
        for part in range(4):
            pack(buf, slot, part * (groups // 4), groups // 4)
        _, early, late = exchange(buf, slot)
        return early + late

    first = begin(load_term, stage_a, ea, 0)
    pl.semaphore_wait(barrier, 8)
    for d in first:
        d.start()
    for d in begin(load_dens, stage_b, ec, 2):
        d.start()
    load_cr.wait()
    in_place(cr)
    for copy in load_fr:
        copy.wait()
    sums[...] = jnp.zeros_like(sums)

    def backward_pair(m, _):
        n = steps - 1 - 2 * m
        stage(ea, eb, 0, 1, n, 1, backward_rows, True, True)
        stage(eb, ea, 1, 0, n - 1, 1, backward_rows, m + 1 < steps // 2, True)
        return 0

    lax.fori_loop(0, steps // 2, backward_pair, 0)
    leave(ea, stage_a, None)
    store_value = pltpu.make_async_copy(stage_a, value_out, load_sem.at[0])
    store_value.start()

    def forward_pair(m, _):
        n = 2 * m
        stage(ec, ea, 2, 0, n, -1, forward_rows, True, False)
        stage(ea, ec, 0, 2, n + 1, -1, forward_rows, m + 1 < steps // 2, False)
        return 0

    lax.fori_loop(0, steps // 2, forward_pair, 0)

    def spread(part, count, at, own, first):
        copies = []
        for hop in range(1, count):
            copies.append(
                pltpu.make_async_remote_copy(
                    src_ref=part.at[0],
                    dst_ref=part.at[hop],
                    send_sem=sum_send.at[first + hop],
                    recv_sem=sum_recv.at[first + hop],
                    device_id=at(lax.rem(own + hop, count)),
                    device_id_type=MESH,
                )
            )
        for copy in copies:
            copy.start()
        for copy in copies:
            copy.wait()
        total = part[0]
        for hop in range(1, count):
            total = total + part[hop]
        return total

    own = [jnp.sum(sums[n], axis=0, keepdims=True) for n in range(steps)]
    part_y[0] = jnp.concatenate(own + [jnp.zeros((8 - steps, LANES), jnp.float32)], axis=0)
    part_x[0] = spread(part_y, ny, lambda j: (x, j), y, 0)
    whole = spread(part_x, nx, lambda i: (i, y), x, ny)
    totals = jnp.sum(whole, axis=1, keepdims=True) * (1.0 / (rows * cols * nx * ny))
    scale = jnp.ones((1, 1), jnp.float32)
    found = []
    for n in range(steps):
        mean = totals[n : n + 1, :] / scale
        found.append(mean)
        scale = scale * (mean + epsilon)
    found.append(jnp.zeros((8 - steps, 1), jnp.float32))
    masses_out[...] = jnp.broadcast_to(jnp.concatenate(found, axis=0), (8, LANES))
    factor = jnp.broadcast_to(1.0 / scale, (BLOCK, cols))

    leave(ec, stage_b, factor)
    store_mass = pltpu.make_async_copy(stage_b, mass_out, load_sem.at[1])
    store_mass.start()
    store_mass.wait()
    store_value.wait()


def shards(terminal, crowding, density, fractions, offsets, control_cost):
    rows, cols = terminal.shape
    tiles = cols // LANES
    steps, controls = control_cost.shape
    nx, ny = lax.axis_size("gx"), lax.axis_size("gy")
    field = jax.ShapeDtypeStruct((rows, cols), jnp.float32)
    tall = rows + 2 * HALO

    def vmem(*shape):
        return pltpu.VMEM(shape, jnp.float32)

    smem = pl.BlockSpec(memory_space=pltpu.SMEM)
    hbm = pl.BlockSpec(memory_space=pl.ANY)
    value, mass, masses = pl.pallas_call(
        kernel,
        out_shape=(field, field, jax.ShapeDtypeStruct((8, LANES), jnp.float32)),
        in_specs=[smem, smem, hbm, hbm, hbm, hbm],
        out_specs=(hbm, hbm, pl.BlockSpec(memory_space=pltpu.VMEM)),
        scratch_shapes=[
            vmem(steps, 8, LANES),
            vmem(ny, 8, LANES),
            vmem(nx, 8, LANES),
            vmem(2 * tiles, tall, LANES),
            vmem(2 * tiles, tall, LANES),
            vmem(2 * tiles, tall, LANES),
            vmem(3, 2, tiles, HALO, LANES),
            vmem(3, 2, tall, LANES),
            vmem(3, 2, rows, LANES),
            vmem(controls, tiles + 3, GROWS, LANES),
            vmem(controls, tiles + 3, GROWS, LANES),
            vmem(tiles, rows // 8, 16, 8, LANES),
            vmem(steps, tiles, rows // 8, controls, 8, LANES),
            vmem(steps, tiles, rows // 8, 8, LANES),
            vmem(rows, cols),
            vmem(steps, 2, rows, cols),
            vmem(rows, cols),
            vmem(rows, cols),
            pltpu.VMEM((cols, cols), jnp.bfloat16),
            pltpu.SemaphoreType.DMA((3 + steps,)),
            pltpu.SemaphoreType.DMA((3, COPIES)),
            pltpu.SemaphoreType.DMA((3, COPIES)),
            pltpu.SemaphoreType.DMA((nx + ny,)),
            pltpu.SemaphoreType.DMA((nx + ny,)),
        ],
        compiler_params=pltpu.CompilerParams(
            collective_id=0, has_side_effects=True, vmem_limit_bytes=60 * 2**20
        ),
    )(jnp.swapaxes(offsets, 1, 2), control_cost, terminal, crowding, density, fractions)
    return value, mass, masses[:steps, 0]


def solution(mesh):
    placed = (P("gx", "gy"), P("gx", "gy"), P("gx", "gy"), P(None, None, "gx", "gy"), P(), P())
    return jax.shard_map(
        shards,
        mesh=mesh,
        in_specs=placed,
        out_specs=(P("gx", "gy"), P("gx", "gy"), P()),
        check_vma=False,
    )
```

```python
import functools

import jax
import jax.numpy as jnp
from jax import lax
from jax.experimental import pallas as pl
from jax.experimental.pallas import tpu as pltpu
from jax.sharding import PartitionSpec as P

MESH = pl.DeviceIdType.MESH
LANES = 128
HALO = 72
PIECE = 24
BLOCK = 128
CHUNK = 64
GROWS = CHUNK + 8
EDGE = 32
LAG = 6
COPIES = 32

time_step = 0.1
temper = 0.3
epsilon = 1e-06


def catmull(t):
    square = t * t
    last = (0.5 * t) * (square - t)
    first = 0.5 * (square - t) - last
    third = 0.5 * (square + t) - 3.0 * last
    second = 1.0 - first - third - last
    return [first, second, third, last]


def kernel(
    off, cost, term, crowd, dens, frac,
    value_out, mass_out, totals_out,
    sums, part_y, part_x, ea, eb, ec, ends, strips, packs, ga, gb,
    wts, ramps, recip, cr, fr, stage_a, stage_b, order,
    load_sem, send_sem, recv_sem, sum_send, sum_recv,
):
    rows, cols = term.shape
    tiles = cols // LANES
    taps = tiles + 3
    groups = rows // 8
    steps, controls = cost.shape
    nx, ny = lax.axis_size("gx"), lax.axis_size("gy")
    x, y = lax.axis_index("gx"), lax.axis_index("gy")
    up, down = lax.rem(x + nx - 1, nx), lax.rem(x + 1, nx)
    left, right = lax.rem(y + ny - 1, ny), lax.rem(y + 1, ny)
    low, high = HALO, HALO + rows

    def lanes_of(count):
        return lax.broadcasted_iota(jnp.int32, (count, LANES), 1)

    load_term = pltpu.make_async_copy(term, stage_a, load_sem.at[0])
    load_dens = pltpu.make_async_copy(dens, stage_b, load_sem.at[1])
    load_cr = pltpu.make_async_copy(crowd, cr, load_sem.at[2])
    load_fr = [
        pltpu.make_async_copy(frac.at[n], fr.at[n], load_sem.at[3 + n]) for n in range(steps)
    ]
    load_term.start()
    load_fr[steps - 1].start()
    load_cr.start()
    load_dens.start()
    for copy in load_fr[: steps - 1]:
        copy.start()

    barrier = pltpu.get_barrier_semaphore()
    around = [(i, j) for i in (up, x, down) for j in (left, y, right)]
    around.pop(4)
    for i, j in around:
        pl.semaphore_signal(barrier, inc=1, device_id=(i, j), device_id_type=MESH)

    def order_rows(i, _):
        here = pl.multiple_of(i * BLOCK, BLOCK)
        source = lax.broadcasted_iota(jnp.int32, (BLOCK, cols), 0) + here
        place = lax.broadcasted_iota(jnp.int32, (BLOCK, cols), 1)
        wanted = tiles * lax.bitwise_and(place, LANES - 1) + lax.shift_right_logical(place, 7)
        order[pl.ds(here, BLOCK), :] = jnp.where(source == wanted, 1.0, 0.0).astype(jnp.bfloat16)
        return 0

    lax.fori_loop(0, cols // BLOCK, order_rows, 0)

    def reorder(value, back):
        count = value.shape[0]
        pieces = []
        rest = value
        for part in range(3):
            pieces.append(rest.astype(jnp.bfloat16))
            if part < 2:
                rest = rest - pieces[-1].astype(jnp.float32)
        got = lax.dot_general(
            jnp.concatenate(pieces, axis=0), order[...], (((1,), (1 if back else 0,)), ((), ())),
            preferred_element_type=jnp.float32,
        )
        return got[:count] + got[count : 2 * count] + got[2 * count :]

    def each_block(body):
        def step(i, _):
            body(pl.multiple_of(i * BLOCK, BLOCK))
            return 0

        lax.fori_loop(0, rows // BLOCK, step, 0)

    def enter(src, buf):
        def body(r):
            got = reorder(src[pl.ds(r, BLOCK), :], False)
            here = pl.ds(pl.multiple_of(HALO + r, 8), BLOCK)
            for c in range(tiles):
                buf[c, here, :] = got[:, c * LANES : (c + 1) * LANES]

        each_block(body)

    def leave(buf, dst):
        def body(r):
            here = pl.ds(pl.multiple_of(HALO + r, 8), BLOCK)
            whole = jnp.concatenate([buf[c, here, :] for c in range(tiles)], axis=1)
            dst[pl.ds(r, BLOCK), :] = reorder(whole, True)

        each_block(body)

    def in_place(ref):
        def body(r):
            ref[pl.ds(r, BLOCK), :] = reorder(ref[pl.ds(r, BLOCK), :], False)

        each_block(body)

    def pack(buf, slot, first, count):
        lane = lanes_of(8 * count)
        here = slice(HALO + 8 * first, HALO + 8 * (first + count))
        there = slice(8 * first, 8 * (first + count))
        tile = [buf[c, here, :] for c in range(tiles)]
        for side in range(2):
            out = None
            for c in range(tiles):
                by = EDGE * (c + side) % LANES
                turned = pltpu.roll(tile[c], by, 1) if by else tile[c]
                out = turned if out is None else jnp.where(lane < EDGE * c, out, turned)
            packs[slot, side, there, :] = out

    def unpack(buf, slot, first, last, turns):
        unit = 8 * (last - first) // turns

        def body(i, _):
            r = pl.ds(pl.multiple_of(first * 8 + i * unit, 8), unit)
            lane = lanes_of(unit)
            near, far = strips[slot, 0, r, :], strips[slot, 1, r, :]
            for c in range(tiles):
                by, bx = (LANES - EDGE * c) % LANES, EDGE * (tiles - 1 - c)
                a = pltpu.roll(near, by, 1) if by else near
                b = pltpu.roll(far, bx, 1) if bx else far
                buf[tiles + c, r, :] = jnp.where(lane < LANES // 2, a, b)
            return 0

        lax.fori_loop(0, turns, body, 0)

    def take_end(buf, slot, side):
        start = (0, high)[side]
        for c in range(tiles):
            buf[c, start : start + HALO, :] = ends[slot, side, c]

    def exchange(buf, slot):
        index = iter(range(COPIES))

        def send(src, dst, i, j):
            at = next(index)
            return pltpu.make_async_remote_copy(
                src_ref=src,
                dst_ref=dst,
                send_sem=send_sem.at[slot, at],
                recv_sem=recv_sem.at[slot, at],
                device_id=(i, j),
                device_id_type=MESH,
            )

        def rows_to(first, count, start, i):
            return [
                send(
                    packs.at[slot, which, pl.ds(first, count), :],
                    strips.at[slot, which, pl.ds(start, count), :],
                    i, j,
                )
                for which, j in ((0, left), (1, right))
            ]

        def north(first, count):
            return [
                send(
                    buf.at[pl.ds(0, tiles), pl.ds(low + first, count), :],
                    ends.at[slot, 1, :, pl.ds(first, count), :],
                    up, y,
                )
            ] + rows_to(first, count, high + first, up)

        def south(first, count):
            start = first - (rows - HALO)
            return [
                send(
                    buf.at[pl.ds(0, tiles), pl.ds(low + first, count), :],
                    ends.at[slot, 0, :, pl.ds(start, count), :],
                    down, y,
                )
            ] + rows_to(first, count, start, down)

        def side(first, count):
            return rows_to(first, count, low + first, x)

        rest, half = HALO - CHUNK, CHUNK // 2
        end_d = [south(rows - CHUNK + part * half, half) for part in range(2)]
        side_d = [side(rows - CHUNK + part * half, half) for part in range(2)]
        end_a = [north(part * half, half) for part in range(2)]
        side_a = [side(part * half, half) for part in range(2)]
        side_c = side(2 * CHUNK - 8, CHUNK + 8)
        top_c = north(CHUNK, rest)
        late_c = side(CHUNK, 8) + south(rows - HALO, rest)
        side_b = side(HALO, CHUNK - 16)
        parts = {
            "d0": end_d[0] + side_d[0],
            "d1": end_d[1] + side_d[1],
            "a0": end_a[0] + side_a[0],
            "a1": end_a[1] + side_a[1],
            "c": side_c + top_c + late_c,
            "b": side_b,
        }
        early = end_a[0] + end_a[1] + top_c + side_d[0] + side_d[1] + side_c
        late = end_d[0] + end_d[1] + side_a[0] + side_a[1] + late_c + side_b
        return parts, early, late

    def weights_pass(n):
        def body(i, _):
            r = pl.ds(pl.multiple_of(i * 8, 8), 8)
            for c in range(tiles):
                lanes = pl.ds(c * LANES, LANES)
                wx = catmull(fr[n, 0, r, lanes])
                wy = catmull(fr[n, 1, r, lanes])
                for a in range(4):
                    for b in range(4):
                        wts[c, i, a * 4 + b] = wx[a] * wy[b]
            return 0

        lax.fori_loop(0, groups, body, 0)

    def shift(src, dst, n, k, row0, sign):
        a, b = sign * off[n, 0, k], sign * off[n, 1, k]
        start = HALO + row0 + a - 1
        lane = lanes_of(PIECE)
        held = {}

        def turn(m, p, first, second, split, amount):
            r = pl.ds(start + p, PIECE)
            both = jnp.where(lane < split, src[first, r, :], src[second, r, :])
            held[m, p] = pltpu.roll(both, amount, 1)

        def put(m, p):
            dst[k, m, p : p + PIECE, :] = held.pop((m, p))

        turns, puts = [], []
        for m in range(taps):
            total = b + (m - 1)
            tile = lax.bitwise_and(total, tiles - 1)
            by = lax.shift_right_arithmetic(total, tiles.bit_length() - 1)
            below = tiles * lax.shift_right_logical(by, 31)
            split = lax.bitwise_and(by, LANES - 1)
            amount = lax.bitwise_and(-by, LANES - 1)
            for p in range(0, GROWS, PIECE):
                turns.append(functools.partial(turn, m, p, tile + tiles - below, tile + below, split, amount))
                puts.append(functools.partial(put, m, p))
        return turns, puts

    def staggered(turns, puts, lag):
        for at in range(len(turns) + lag):
            now = []
            if at < len(turns):
                now.append(turns[at])
            if at >= lag:
                now.append(puts[at - lag])
            yield now

    def weave(main, side):
        done = 0
        for at, step in enumerate(main):
            step()
            due = (at + 1) * len(side) // len(main)
            for i in range(done, due):
                for one in side[i]:
                    one()
            done = due

    def sample(src, w, k, c, j):
        acc = None
        for a in range(4):
            for b in range(4):
                part = w[a * 4 + b] * src[k, c + b, pl.ds(j + a, 8), :]
                acc = part if acc is None else acc + part
        return acc

    def backward_rows(src, dst, n, row0, i):
        j = pl.multiple_of(i * 8, 8)
        g = row0 // 8 + i
        r = pl.ds(pl.multiple_of(row0 + j, 8), 8)
        here = pl.ds(pl.multiple_of(HALO + row0 + j, 8), 8)
        out = []
        for c in range(tiles):
            w, q = [], []

            def take(k, c=c, w=w, q=q):
                if k == 0:
                    w.extend(wts[c, g, m] for m in range(16))
                q.append(sample(src, w, k, c, j) + time_step * cost[n, k])
                if k == controls - 1:
                    lowest = functools.reduce(jnp.minimum, q)
                    edge = lowest + temper
                    total = None
                    for kk in range(controls):
                        ramp = jnp.maximum(edge - q[kk], 0.0)
                        ramps[n, c, g, kk] = ramp
                        total = ramp if total is None else total + ramp
                    recip[n, c, g] = 1.0 / total
                    dst[c, here, :] = lowest + time_step * cr[r, pl.ds(c * LANES, LANES)]

            out += [functools.partial(take, k) for k in range(controls)]
        return out

    def forward_rows(src, dst, n, row0, i):
        j = pl.multiple_of(i * 8, 8)
        g = row0 // 8 + i
        here = pl.ds(pl.multiple_of(HALO + row0 + j, 8), 8)
        out, added = [], []
        for c in range(tiles):
            w, acc = [], []

            def take(k, c=c, w=w, acc=acc):
                if k == 0:
                    w.extend(wts[c, g, m] for m in range(16))
                part = ramps[n, c, g, k] * sample(src, w, k, c, j)
                acc.append(part if k == 0 else acc[-1] + part)
                if k == controls - 1:
                    arrived = jnp.maximum(acc[-1] * recip[n, c, g], 0.0)
                    dst[c, here, :] = arrived
                    added.append(arrived)
                    if c == tiles - 1:
                        sums[n] = sums[n] + functools.reduce(jnp.add, added)

            out += [functools.partial(take, k) for k in range(controls)]
        return out

    per = CHUNK // 8
    mine = {"d": rows - CHUNK, "a": 0, "c": 2 * CHUNK, "b": CHUNK}

    def stage(src, dst, slot_src, slot_dst, n, sign, rows_fn, send, fresh):
        if fresh:
            in_place(fr.at[n, 0])
            in_place(fr.at[n, 1])
        weights_pass(n)
        _, early, late = exchange(src, slot_src)
        for d in early:
            d.wait()
        unpack(src, slot_src, 2 * (low // 8) + 6, (high + HALO) // 8, 2)
        take_end(src, slot_src, 1)

        def first(k, _):
            one, two = (shift(src, ga, n, 2 * k + u, mine["d"], sign) for u in range(2))
            for now in staggered(one[0] + two[0], one[1] + two[1], 20):
                for step in now:
                    step()
            return 0

        lax.fori_loop(0, controls // 2, first, 0)
        for d in late:
            d.wait()
        unpack(src, slot_src, 0, 2 * (low // 8) + 6, 3)
        take_end(src, slot_src, 0)
        parts, _, _ = exchange(dst, slot_dst)

        def put_out(name, pieces):
            for at, count in pieces:
                pack(dst, slot_dst, at, count)
            for d in parts[name]:
                d.start()

        def publish(name, pieces):
            if send is True:
                put_out(name, pieces)
            else:
                pl.when(send)(functools.partial(put_out, name, pieces))

        def block(now, later, name, following, start, stop, place, halves=False):
            def body(i, _):
                side = []
                if following is not None:
                    side = list(staggered(*shift(src, later, n, i, mine[following], sign), LAG))
                weave(rows_fn(now, dst, n, mine[name], place(i)), side)
                if halves:
                    for part in range(2):
                        ready = i == (part + 1) * per // 2 - 1
                        if send is not True:
                            ready = jnp.logical_and(ready, send)
                        at = mine[name] // 8 + part * (per // 2)

                        @pl.when(ready)
                        def _(part=part, at=at):
                            put_out(f"{name}{part}", [(at, per // 2)])

                return 0

            lax.fori_loop(start, stop, body, 0)

        def plain(i):
            return i

        block(ga, gb, "d", "a", 0, per, plain, True)
        block(gb, ga, "a", "c", 0, per, plain, True)
        block(ga, gb, "c", "b", 0, per, plain)
        block(gb, None, "b", None, 0, 2, lambda i: (per - 1) * (1 - i))
        publish("c", [(mine["c"] // 8 - 1, per + 1), (per, 1)])
        block(gb, None, "b", None, 1, per - 1, plain)
        publish("b", [(per + 1, per - 2)])

    def begin(load, src, buf, slot):
        load.wait()
        enter(src, buf)
        for part in range(4):
            pack(buf, slot, part * (groups // 4), groups // 4)
        _, early, late = exchange(buf, slot)
        return early + late

    first = begin(load_term, stage_a, ea, 0)
    pl.semaphore_wait(barrier, 8)
    for d in first:
        d.start()
    for d in begin(load_dens, stage_b, ec, 2):
        d.start()
    load_cr.wait()
    in_place(cr)
    for copy in load_fr:
        copy.wait()
    sums[...] = jnp.zeros_like(sums)

    def backward_pair(m, _):
        n = steps - 1 - 2 * m
        stage(ea, eb, 0, 1, n, 1, backward_rows, True, True)
        stage(eb, ea, 1, 0, n - 1, 1, backward_rows, m + 1 < steps // 2, True)
        return 0

    lax.fori_loop(0, steps // 2, backward_pair, 0)
    leave(ea, stage_a)
    store_value = pltpu.make_async_copy(stage_a, value_out, load_sem.at[0])
    store_value.start()

    def forward_pair(m, _):
        n = 2 * m
        stage(ec, ea, 2, 0, n, -1, forward_rows, True, False)
        stage(ea, ec, 0, 2, n + 1, -1, forward_rows, m + 1 < steps // 2, False)
        return 0

    lax.fori_loop(0, steps // 2, forward_pair, 0)

    def spread(part, count, at, own, first):
        copies = []
        for hop in range(1, count):
            copies.append(
                pltpu.make_async_remote_copy(
                    src_ref=part.at[0],
                    dst_ref=part.at[hop],
                    send_sem=sum_send.at[first + hop],
                    recv_sem=sum_recv.at[first + hop],
                    device_id=at(lax.rem(own + hop, count)),
                    device_id_type=MESH,
                )
            )
        for copy in copies:
            copy.start()

        def finish():
            for copy in copies:
                copy.wait()
            total = part[0]
            for hop in range(1, count):
                total = total + part[hop]
            return total

        return finish

    own = [jnp.sum(sums[n], axis=0, keepdims=True) for n in range(steps)]
    part_y[0] = jnp.concatenate(own + [jnp.zeros((8 - steps, LANES), jnp.float32)], axis=0)
    finish_y = spread(part_y, ny, lambda j: (x, j), y, 0)
    leave(ec, stage_b)
    store_mass = pltpu.make_async_copy(stage_b, mass_out, load_sem.at[1])
    store_mass.start()
    part_x[0] = finish_y()
    finish_x = spread(part_x, nx, lambda i: (i, y), x, ny)
    store_mass.wait()
    store_value.wait()
    whole = finish_x()
    totals = jnp.sum(whole, axis=1, keepdims=True) * (1.0 / (rows * cols * nx * ny))
    totals_out[...] = jnp.broadcast_to(totals, (8, LANES))


def finish_kernel(value, mass, totals, value_out, mass_out, masses_out):
    steps = masses_out.shape[0]
    scale = jnp.float32(1.0)
    for n in range(steps):
        mean = totals[n, 0] / scale
        masses_out[n] = mean
        scale = scale * (mean + epsilon)
    factor = 1.0 / jnp.full(mass.shape, scale, jnp.float32)
    value_out[...] = value[...]
    mass_out[...] = mass[...] * factor


def shards(terminal, crowding, density, fractions, offsets, control_cost):
    rows, cols = terminal.shape
    tiles = cols // LANES
    steps, controls = control_cost.shape
    nx, ny = lax.axis_size("gx"), lax.axis_size("gy")
    field = jax.ShapeDtypeStruct((rows, cols), jnp.float32)
    tall = rows + 2 * HALO

    def vmem(*shape):
        return pltpu.VMEM(shape, jnp.float32)

    smem = pl.BlockSpec(memory_space=pltpu.SMEM)
    hbm = pl.BlockSpec(memory_space=pl.ANY)
    value, mass, totals = pl.pallas_call(
        kernel,
        out_shape=(field, field, jax.ShapeDtypeStruct((8, LANES), jnp.float32)),
        in_specs=[smem, smem, hbm, hbm, hbm, hbm],
        out_specs=(hbm, hbm, pl.BlockSpec(memory_space=pltpu.VMEM)),
        scratch_shapes=[
            vmem(steps, 8, LANES),
            vmem(ny, 8, LANES),
            vmem(nx, 8, LANES),
            vmem(2 * tiles, tall, LANES),
            vmem(2 * tiles, tall, LANES),
            vmem(2 * tiles, tall, LANES),
            vmem(3, 2, tiles, HALO, LANES),
            vmem(3, 2, tall, LANES),
            vmem(3, 2, rows, LANES),
            vmem(controls, tiles + 3, GROWS, LANES),
            vmem(controls, tiles + 3, GROWS, LANES),
            vmem(tiles, rows // 8, 16, 8, LANES),
            vmem(steps, tiles, rows // 8, controls, 8, LANES),
            vmem(steps, tiles, rows // 8, 8, LANES),
            vmem(rows, cols),
            vmem(steps, 2, rows, cols),
            vmem(rows, cols),
            vmem(rows, cols),
            pltpu.VMEM((cols, cols), jnp.bfloat16),
            pltpu.SemaphoreType.DMA((3 + steps,)),
            pltpu.SemaphoreType.DMA((3, COPIES)),
            pltpu.SemaphoreType.DMA((3, COPIES)),
            pltpu.SemaphoreType.DMA((nx + ny,)),
            pltpu.SemaphoreType.DMA((nx + ny,)),
        ],
        compiler_params=pltpu.CompilerParams(
            collective_id=0, has_side_effects=True, vmem_limit_bytes=60 * 2**20
        ),
    )(jnp.swapaxes(offsets, 1, 2), control_cost, terminal, crowding, density, fractions)
    whole = pl.BlockSpec(memory_space=pltpu.VMEM)
    return pl.pallas_call(
        finish_kernel,
        out_shape=(field, field, jax.ShapeDtypeStruct((steps,), jnp.float32)),
        in_specs=[whole, whole, smem],
        out_specs=(whole, whole, smem),
    )(value, mass, totals)


def solution(mesh):
    placed = (P("gx", "gy"), P("gx", "gy"), P("gx", "gy"), P(None, None, "gx", "gy"), P(), P())
    return jax.shard_map(
        shards,
        mesh=mesh,
        in_specs=placed,
        out_specs=(P("gx", "gy"), P("gx", "gy"), P()),
        check_vma=False,
    )
```

```python
import functools

import jax
import jax.numpy as jnp
from jax import lax
from jax.experimental import pallas as pl
from jax.experimental.pallas import tpu as pltpu
from jax.sharding import PartitionSpec as P

MESH = pl.DeviceIdType.MESH
LANES = 128
HALO = 72
PIECE = 72
BLOCK = 128
CHUNK = 64
GROWS = CHUNK + 8
EDGE = 32
LAG = 2
COPIES = 32

time_step = 0.1
temper = 0.3
epsilon = 1e-06


def catmull(t):
    square = t * t
    last = (0.5 * t) * (square - t)
    first = 0.5 * (square - t) - last
    third = 0.5 * (square + t) - 3.0 * last
    second = 1.0 - first - third - last
    return [first, second, third, last]


def kernel(
    off, cost, term, crowd, dens, frac,
    value_out, mass_out, totals_out,
    sums, part_y, part_x, ea, eb, ec, ends, strips, packs, ga, gb,
    wts, ramps, recip, cr, fr, stage_a, stage_b, order,
    load_sem, send_sem, recv_sem, sum_send, sum_recv,
):
    rows, cols = term.shape
    tiles = cols // LANES
    taps = tiles + 3
    groups = rows // 8
    steps, controls = cost.shape
    nx, ny = lax.axis_size("gx"), lax.axis_size("gy")
    x, y = lax.axis_index("gx"), lax.axis_index("gy")
    up, down = lax.rem(x + nx - 1, nx), lax.rem(x + 1, nx)
    left, right = lax.rem(y + ny - 1, ny), lax.rem(y + 1, ny)
    low, high = HALO, HALO + rows

    def lanes_of(count):
        return lax.broadcasted_iota(jnp.int32, (count, LANES), 1)

    load_term = pltpu.make_async_copy(term, stage_a, load_sem.at[0])
    load_dens = pltpu.make_async_copy(dens, stage_b, load_sem.at[1])
    load_cr = pltpu.make_async_copy(crowd, cr, load_sem.at[2])
    load_fr = [
        pltpu.make_async_copy(frac.at[n], fr.at[n], load_sem.at[3 + n]) for n in range(steps)
    ]
    load_term.start()
    load_fr[steps - 1].start()
    load_cr.start()
    load_dens.start()
    for copy in load_fr[: steps - 1]:
        copy.start()

    barrier = pltpu.get_barrier_semaphore()
    around = [(i, j) for i in (up, x, down) for j in (left, y, right)]
    around.pop(4)
    for i, j in around:
        pl.semaphore_signal(barrier, inc=1, device_id=(i, j), device_id_type=MESH)

    def order_rows(i, _):
        here = pl.multiple_of(i * BLOCK, BLOCK)
        source = lax.broadcasted_iota(jnp.int32, (BLOCK, cols), 0) + here
        place = lax.broadcasted_iota(jnp.int32, (BLOCK, cols), 1)
        wanted = tiles * lax.bitwise_and(place, LANES - 1) + lax.shift_right_logical(place, 7)
        order[pl.ds(here, BLOCK), :] = jnp.where(source == wanted, 1.0, 0.0).astype(jnp.bfloat16)
        return 0

    lax.fori_loop(0, cols // BLOCK, order_rows, 0)

    def reorder(value, back):
        count = value.shape[0]
        pieces = []
        rest = value
        for part in range(3):
            pieces.append(rest.astype(jnp.bfloat16))
            if part < 2:
                rest = rest - pieces[-1].astype(jnp.float32)
        got = lax.dot_general(
            jnp.concatenate(pieces, axis=0), order[...], (((1,), (1 if back else 0,)), ((), ())),
            preferred_element_type=jnp.float32,
        )
        return got[:count] + got[count : 2 * count] + got[2 * count :]

    def each_block(body):
        def step(i, _):
            body(pl.multiple_of(i * BLOCK, BLOCK))
            return 0

        lax.fori_loop(0, rows // BLOCK, step, 0)

    def enter(src, buf):
        def body(r):
            got = reorder(src[pl.ds(r, BLOCK), :], False)
            here = pl.ds(pl.multiple_of(HALO + r, 8), BLOCK)
            for c in range(tiles):
                buf[c, here, :] = got[:, c * LANES : (c + 1) * LANES]

        each_block(body)

    def leave(buf, dst):
        def body(r):
            here = pl.ds(pl.multiple_of(HALO + r, 8), BLOCK)
            whole = jnp.concatenate([buf[c, here, :] for c in range(tiles)], axis=1)
            dst[pl.ds(r, BLOCK), :] = reorder(whole, True)

        each_block(body)

    def in_place(ref):
        def body(r):
            ref[pl.ds(r, BLOCK), :] = reorder(ref[pl.ds(r, BLOCK), :], False)

        each_block(body)

    def pack(buf, slot, first, count):
        lane = lanes_of(8 * count)
        here = slice(HALO + 8 * first, HALO + 8 * (first + count))
        there = slice(8 * first, 8 * (first + count))
        tile = [buf[c, here, :] for c in range(tiles)]
        for side in range(2):
            out = None
            for c in range(tiles):
                by = EDGE * (c + side) % LANES
                turned = pltpu.roll(tile[c], by, 1) if by else tile[c]
                out = turned if out is None else jnp.where(lane < EDGE * c, out, turned)
            packs[slot, side, there, :] = out

    def unpack(buf, slot, first, last, turns):
        unit = 8 * (last - first) // turns

        def body(i, _):
            r = pl.ds(pl.multiple_of(first * 8 + i * unit, 8), unit)
            lane = lanes_of(unit)
            near, far = strips[slot, 0, r, :], strips[slot, 1, r, :]
            for c in range(tiles):
                by, bx = (LANES - EDGE * c) % LANES, EDGE * (tiles - 1 - c)
                a = pltpu.roll(near, by, 1) if by else near
                b = pltpu.roll(far, bx, 1) if bx else far
                buf[tiles + c, r, :] = jnp.where(lane < LANES // 2, a, b)
            return 0

        lax.fori_loop(0, turns, body, 0)

    def take_end(buf, slot, side):
        start = (0, high)[side]
        for c in range(tiles):
            buf[c, start : start + HALO, :] = ends[slot, side, c]

    def exchange(buf, slot, down_last):
        index = iter(range(COPIES))

        def send(src, dst, i, j):
            at = next(index)
            return pltpu.make_async_remote_copy(
                src_ref=src,
                dst_ref=dst,
                send_sem=send_sem.at[slot, at],
                recv_sem=recv_sem.at[slot, at],
                device_id=(i, j),
                device_id_type=MESH,
            )

        def rows_to(first, count, start, i):
            return [
                send(
                    packs.at[slot, which, pl.ds(first, count), :],
                    strips.at[slot, which, pl.ds(start, count), :],
                    i, j,
                )
                for which, j in ((0, left), (1, right))
            ]

        def north(first, count):
            return [
                send(
                    buf.at[pl.ds(0, tiles), pl.ds(low + first, count), :],
                    ends.at[slot, 1, :, pl.ds(first, count), :],
                    up, y,
                )
            ] + rows_to(first, count, high + first, up)

        def south(first, count):
            start = first - (rows - HALO)
            return [
                send(
                    buf.at[pl.ds(0, tiles), pl.ds(low + first, count), :],
                    ends.at[slot, 0, :, pl.ds(start, count), :],
                    down, y,
                )
            ] + rows_to(first, count, start, down)

        def side(first, count):
            return rows_to(first, count, low + first, x)

        rest, half = HALO - CHUNK, CHUNK // 2
        end_d = [south(rows - CHUNK + part * half, half) for part in range(2)]
        side_d = [side(rows - CHUNK + part * half, half) for part in range(2)]
        end_a = [north(part * half, half) for part in range(2)]
        side_a = [side(part * half, half) for part in range(2)]
        if down_last:
            first_m = side(CHUNK, CHUNK + 8) + south(rows - HALO, rest)
            later_m = side(rows - HALO, rest) + north(CHUNK, rest)
            side_z = side(2 * CHUNK + 8, CHUNK - 16)
        else:
            first_m = side(2 * CHUNK - 8, CHUNK + 8) + north(CHUNK, rest)
            later_m = side(CHUNK, rest) + south(rows - HALO, rest)
            side_z = side(HALO, CHUNK - 16)
        parts = {
            "d0": end_d[0] + side_d[0],
            "d1": end_d[1] + side_d[1],
            "a0": end_a[0] + side_a[0],
            "a1": end_a[1] + side_a[1],
            "m": first_m + later_m,
            "z": side_z,
        }
        ends_d, ends_a = end_d[0] + end_d[1], end_a[0] + end_a[1]
        sides_d, sides_a = side_d[0] + side_d[1], side_a[0] + side_a[1]
        if down_last:
            early, late = ends_d + sides_a, ends_a + sides_d
        else:
            early, late = ends_a + sides_d, ends_d + sides_a
        early, late = early + first_m, late + later_m + side_z
        return parts, early, late

    def weights_pass(n):
        def body(i, _):
            r = pl.ds(pl.multiple_of(i * 8, 8), 8)
            for c in range(tiles):
                lanes = pl.ds(c * LANES, LANES)
                wx = catmull(fr[n, 0, r, lanes])
                wy = catmull(fr[n, 1, r, lanes])
                for a in range(4):
                    for b in range(4):
                        wts[c, i, a * 4 + b] = wx[a] * wy[b]
            return 0

        lax.fori_loop(0, groups, body, 0)

    def shift(src, dst, n, k, row0, sign):
        a, b = sign * off[n, 0, k], sign * off[n, 1, k]
        start = HALO + row0 + a - 1
        lane = lanes_of(PIECE)
        held = {}

        def turn(m, p, first, second, split, amount):
            r = pl.ds(start + p, PIECE)
            both = jnp.where(lane < split, src[first, r, :], src[second, r, :])
            held[m, p] = pltpu.roll(both, amount, 1)

        def put(m, p):
            dst[k, m, p : p + PIECE, :] = held.pop((m, p))

        turns, puts = [], []
        for m in range(taps):
            total = b + (m - 1)
            tile = lax.bitwise_and(total, tiles - 1)
            by = lax.shift_right_arithmetic(total, tiles.bit_length() - 1)
            below = tiles * lax.shift_right_logical(by, 31)
            split = lax.bitwise_and(by, LANES - 1)
            amount = lax.bitwise_and(-by, LANES - 1)
            for p in range(0, GROWS, PIECE):
                turns.append(functools.partial(turn, m, p, tile + tiles - below, tile + below, split, amount))
                puts.append(functools.partial(put, m, p))
        return turns, puts

    def staggered(turns, puts, lag):
        for at in range(len(turns) + lag):
            now = []
            if at < len(turns):
                now.append(turns[at])
            if at >= lag:
                now.append(puts[at - lag])
            yield now

    def weave(main, side):
        done = 0
        for at, step in enumerate(main):
            step()
            due = (at + 1) * len(side) // len(main)
            for i in range(done, due):
                for one in side[i]:
                    one()
            done = due

    def sample(src, w, k, c, j):
        acc = None
        for a in range(4):
            for b in range(4):
                part = w[a * 4 + b] * src[k, c + b, pl.ds(j + a, 8), :]
                acc = part if acc is None else acc + part
        return acc

    def backward_rows(src, dst, n, row0, i):
        j = pl.multiple_of(i * 8, 8)
        g = row0 // 8 + i
        r = pl.ds(pl.multiple_of(row0 + j, 8), 8)
        here = pl.ds(pl.multiple_of(HALO + row0 + j, 8), 8)
        out = []
        for c in range(tiles):
            w, q = [], []

            def take(k, c=c, w=w, q=q):
                if k == 0:
                    w.extend(wts[c, g, m] for m in range(16))
                q.append(sample(src, w, k, c, j) + time_step * cost[n, k])
                if k == controls - 1:
                    lowest = functools.reduce(jnp.minimum, q)
                    edge = lowest + temper
                    total = None
                    for kk in range(controls):
                        ramp = jnp.maximum(edge - q[kk], 0.0)
                        ramps[n, c, g, kk] = ramp
                        total = ramp if total is None else total + ramp
                    recip[n, c, g] = 1.0 / total
                    dst[c, here, :] = lowest + time_step * cr[r, pl.ds(c * LANES, LANES)]

            out += [functools.partial(take, k) for k in range(controls)]
        return out

    def forward_rows(src, dst, n, row0, i):
        j = pl.multiple_of(i * 8, 8)
        g = row0 // 8 + i
        here = pl.ds(pl.multiple_of(HALO + row0 + j, 8), 8)
        out, added = [], []
        for c in range(tiles):
            w, q = [], []

            def take(k, c=c, w=w, q=q):
                if k == 0:
                    w.extend(wts[c, g, m] for m in range(16))
                q.append(sample(src, w, k, c, j))
                if k == controls - 1:
                    acc = None
                    for kk in range(controls):
                        part = ramps[n, c, g, kk] * q[kk]
                        acc = part if acc is None else acc + part
                    arrived = jnp.maximum(acc * recip[n, c, g], 0.0)
                    dst[c, here, :] = arrived
                    added.append(arrived)
                    if c == tiles - 1:
                        sums[n] = sums[n] + functools.reduce(jnp.add, added)

            out += [functools.partial(take, k) for k in range(controls)]
        return out

    per = CHUNK // 8
    mine = {"d": rows - CHUNK, "a": 0, "c": 2 * CHUNK, "b": CHUNK}

    def stage(src, dst, slot_src, slot_dst, n, sign, rows_fn, send, fresh, d_first):
        if fresh:
            in_place(fr.at[n, 0])
            in_place(fr.at[n, 1])
        weights_pass(n)
        _, early, late = exchange(src, slot_src, not d_first)
        for d in early:
            d.wait()
        all_rows, cut = (high + HALO) // 8, 13 * 2
        if d_first:
            unpack(src, slot_src, all_rows - cut, all_rows, 2)
        else:
            unpack(src, slot_src, 0, cut, 2)
        take_end(src, slot_src, 1 if d_first else 0)

        def first(k, _):
            one, two = (shift(src, ga, n, 2 * k + u, mine["d" if d_first else "a"], sign) for u in range(2))
            for now in staggered(one[0] + two[0], one[1] + two[1], 20):
                for step in now:
                    step()
            return 0

        lax.fori_loop(0, controls // 2, first, 0)
        for d in late:
            d.wait()
        if d_first:
            unpack(src, slot_src, 0, all_rows - cut, 3)
        else:
            unpack(src, slot_src, cut, all_rows, 3)
        take_end(src, slot_src, 0 if d_first else 1)
        parts, _, _ = exchange(dst, slot_dst, d_first)

        def put_out(name, pieces):
            for at, count in pieces:
                pack(dst, slot_dst, at, count)
            for d in parts[name]:
                d.start()

        def publish(name, pieces):
            if send is True:
                put_out(name, pieces)
            else:
                pl.when(send)(functools.partial(put_out, name, pieces))

        def block(now, later, name, following, start, stop, place, halves=False):
            def body(i, _):
                side = []
                if following is not None:
                    side = list(staggered(*shift(src, later, n, i, mine[following], sign), LAG))
                weave(rows_fn(now, dst, n, mine[name], place(i)), side)
                if halves:
                    for part in range(2):
                        ready = i == (part + 1) * per // 2 - 1
                        if send is not True:
                            ready = jnp.logical_and(ready, send)
                        at = mine[name] // 8 + part * (per // 2)

                        @pl.when(ready)
                        def _(part=part, at=at):
                            put_out(f"{name}{part}", [(at, per // 2)])

                return 0

            lax.fori_loop(start, stop, body, 0)

        def plain(i):
            return i

        turn = "dabc" if d_first else "adcb"
        block(ga, gb, turn[0], turn[1], 0, per, plain, True)
        block(gb, ga, turn[1], turn[2], 0, per, plain, True)
        block(ga, gb, turn[2], turn[3], 0, per, plain)
        block(gb, None, turn[3], None, 0, 2, lambda i: (per - 1) * (1 - i))
        last = mine[turn[3]] // 8
        if d_first:
            publish("m", [(per, per + 1), (last + per - 1, 1)])
        else:
            publish("m", [(mine["c"] // 8 - 1, per + 1), (last, 1)])
        block(gb, None, turn[3], None, 1, per - 1, plain)
        publish("z", [(last + 1, per - 2)])

    def begin(load, src, buf, slot):
        load.wait()
        enter(src, buf)
        for part in range(4):
            pack(buf, slot, part * (groups // 4), groups // 4)
        _, early, late = exchange(buf, slot, False)
        return early + late

    first = begin(load_term, stage_a, ea, 0)
    pl.semaphore_wait(barrier, 8)
    for d in first:
        d.start()
    for d in begin(load_dens, stage_b, ec, 2):
        d.start()
    load_cr.wait()
    in_place(cr)
    for copy in load_fr:
        copy.wait()
    sums[...] = jnp.zeros_like(sums)

    def backward_pair(m, _):
        n = steps - 1 - 2 * m
        stage(ea, eb, 0, 1, n, 1, backward_rows, True, True, True)
        stage(eb, ea, 1, 0, n - 1, 1, backward_rows, m + 1 < steps // 2, True, False)
        return 0

    lax.fori_loop(0, steps // 2, backward_pair, 0)
    leave(ea, stage_a)
    store_value = pltpu.make_async_copy(stage_a, value_out, load_sem.at[0])
    store_value.start()

    def forward_pair(m, _):
        n = 2 * m
        stage(ec, ea, 2, 0, n, -1, forward_rows, True, False, True)
        stage(ea, ec, 0, 2, n + 1, -1, forward_rows, m + 1 < steps // 2, False, False)
        return 0

    lax.fori_loop(0, steps // 2, forward_pair, 0)

    def spread(part, count, at, own, first):
        copies = []
        for hop in range(1, count):
            copies.append(
                pltpu.make_async_remote_copy(
                    src_ref=part.at[0],
                    dst_ref=part.at[hop],
                    send_sem=sum_send.at[first + hop],
                    recv_sem=sum_recv.at[first + hop],
                    device_id=at(lax.rem(own + hop, count)),
                    device_id_type=MESH,
                )
            )
        for copy in copies:
            copy.start()

        def finish():
            for copy in copies:
                copy.wait()
            total = part[0]
            for hop in range(1, count):
                total = total + part[hop]
            return total

        return finish

    own = [jnp.sum(sums[n], axis=0, keepdims=True) for n in range(steps)]
    part_y[0] = jnp.concatenate(own + [jnp.zeros((8 - steps, LANES), jnp.float32)], axis=0)
    finish_y = spread(part_y, ny, lambda j: (x, j), y, 0)
    leave(ec, stage_b)
    store_mass = pltpu.make_async_copy(stage_b, mass_out, load_sem.at[1])
    store_mass.start()
    part_x[0] = finish_y()
    finish_x = spread(part_x, nx, lambda i: (i, y), x, ny)
    store_mass.wait()
    store_value.wait()
    whole = finish_x()
    totals = jnp.sum(whole, axis=1, keepdims=True) * (1.0 / (rows * cols * nx * ny))
    totals_out[...] = jnp.broadcast_to(totals, (8, LANES))


def finish_kernel(value, mass, totals, value_out, mass_out, masses_out):
    steps = masses_out.shape[0]
    scale = jnp.float32(1.0)
    for n in range(steps):
        mean = totals[n, 0] / scale
        masses_out[n] = mean
        scale = scale * (mean + epsilon)
    factor = 1.0 / jnp.full(mass.shape, scale, jnp.float32)
    value_out[...] = value[...]
    mass_out[...] = mass[...] * factor


def shards(terminal, crowding, density, fractions, offsets, control_cost):
    rows, cols = terminal.shape
    tiles = cols // LANES
    steps, controls = control_cost.shape
    nx, ny = lax.axis_size("gx"), lax.axis_size("gy")
    field = jax.ShapeDtypeStruct((rows, cols), jnp.float32)
    tall = rows + 2 * HALO

    def vmem(*shape):
        return pltpu.VMEM(shape, jnp.float32)

    smem = pl.BlockSpec(memory_space=pltpu.SMEM)
    hbm = pl.BlockSpec(memory_space=pl.ANY)
    value, mass, totals = pl.pallas_call(
        kernel,
        out_shape=(field, field, jax.ShapeDtypeStruct((8, LANES), jnp.float32)),
        in_specs=[smem, smem, hbm, hbm, hbm, hbm],
        out_specs=(hbm, hbm, pl.BlockSpec(memory_space=pltpu.VMEM)),
        scratch_shapes=[
            vmem(steps, 8, LANES),
            vmem(ny, 8, LANES),
            vmem(nx, 8, LANES),
            vmem(2 * tiles, tall, LANES),
            vmem(2 * tiles, tall, LANES),
            vmem(2 * tiles, tall, LANES),
            vmem(3, 2, tiles, HALO, LANES),
            vmem(3, 2, tall, LANES),
            vmem(3, 2, rows, LANES),
            vmem(controls, tiles + 3, GROWS, LANES),
            vmem(controls, tiles + 3, GROWS, LANES),
            vmem(tiles, rows // 8, 16, 8, LANES),
            vmem(steps, tiles, rows // 8, controls, 8, LANES),
            vmem(steps, tiles, rows // 8, 8, LANES),
            vmem(rows, cols),
            vmem(steps, 2, rows, cols),
            vmem(rows, cols),
            vmem(rows, cols),
            pltpu.VMEM((cols, cols), jnp.bfloat16),
            pltpu.SemaphoreType.DMA((3 + steps,)),
            pltpu.SemaphoreType.DMA((3, COPIES)),
            pltpu.SemaphoreType.DMA((3, COPIES)),
            pltpu.SemaphoreType.DMA((nx + ny,)),
            pltpu.SemaphoreType.DMA((nx + ny,)),
        ],
        compiler_params=pltpu.CompilerParams(
            collective_id=0, has_side_effects=True, vmem_limit_bytes=60 * 2**20
        ),
    )(jnp.swapaxes(offsets, 1, 2), control_cost, terminal, crowding, density, fractions)
    whole = pl.BlockSpec(memory_space=pltpu.VMEM)
    return pl.pallas_call(
        finish_kernel,
        out_shape=(field, field, jax.ShapeDtypeStruct((steps,), jnp.float32)),
        in_specs=[whole, whole, smem],
        out_specs=(whole, whole, smem),
    )(value, mass, totals)


def solution(mesh):
    placed = (P("gx", "gy"), P("gx", "gy"), P("gx", "gy"), P(None, None, "gx", "gy"), P(), P())
    return jax.shard_map(
        shards,
        mesh=mesh,
        in_specs=placed,
        out_specs=(P("gx", "gy"), P("gx", "gy"), P()),
        check_vma=False,
    )
```

```python
import functools

import jax
import jax.numpy as jnp
from jax import lax
from jax.experimental import pallas as pl
from jax.experimental.pallas import tpu as pltpu
from jax.sharding import PartitionSpec as P

MESH = pl.DeviceIdType.MESH
LANES = 128
HALO = 72
PIECE = 72
BLOCK = 128
CHUNK = 64
GROWS = CHUNK + 8
EDGE = 32
LAG = 2
COPIES = 32

time_step = 0.1
temper = 0.3
epsilon = 1e-06


def catmull(t):
    square = t * t
    last = (0.5 * t) * (square - t)
    first = 0.5 * (square - t) - last
    third = 0.5 * (square + t) - 3.0 * last
    second = 1.0 - first - third - last
    return [first, second, third, last]


def kernel(
    off, cost, term, crowd, dens, frac,
    value_out, mass_out, totals_out,
    sums, part_y, part_x, ea, eb, ec, ends, strips, packs, ga, gb,
    wts, ramps, recip, cr, fr, stage_a, stage_b, order,
    load_sem, send_sem, recv_sem, sum_send, sum_recv,
):
    rows, cols = term.shape
    tiles = cols // LANES
    taps = tiles + 3
    groups = rows // 8
    steps, controls = cost.shape
    nx, ny = lax.axis_size("gx"), lax.axis_size("gy")
    x, y = lax.axis_index("gx"), lax.axis_index("gy")
    up, down = lax.rem(x + nx - 1, nx), lax.rem(x + 1, nx)
    left, right = lax.rem(y + ny - 1, ny), lax.rem(y + 1, ny)
    low, high = HALO, HALO + rows

    def lanes_of(count):
        return lax.broadcasted_iota(jnp.int32, (count, LANES), 1)

    load_term = pltpu.make_async_copy(term, stage_a, load_sem.at[0])
    load_dens = pltpu.make_async_copy(dens, stage_b, load_sem.at[1])
    load_cr = pltpu.make_async_copy(crowd, cr, load_sem.at[2])
    load_fr = [
        pltpu.make_async_copy(frac.at[n], fr.at[n], load_sem.at[3 + n]) for n in range(steps)
    ]
    load_term.start()
    load_fr[steps - 1].start()
    load_cr.start()
    load_dens.start()
    for copy in load_fr[: steps - 1]:
        copy.start()

    barrier = pltpu.get_barrier_semaphore()
    around = [(i, j) for i in (up, x, down) for j in (left, y, right)]
    around.pop(4)
    for i, j in around:
        pl.semaphore_signal(barrier, inc=1, device_id=(i, j), device_id_type=MESH)

    def order_rows(i, _):
        here = pl.multiple_of(i * BLOCK, BLOCK)
        source = lax.broadcasted_iota(jnp.int32, (BLOCK, cols), 0) + here
        place = lax.broadcasted_iota(jnp.int32, (BLOCK, cols), 1)
        wanted = tiles * lax.bitwise_and(place, LANES - 1) + lax.shift_right_logical(place, 7)
        order[pl.ds(here, BLOCK), :] = jnp.where(source == wanted, 1.0, 0.0).astype(jnp.bfloat16)
        return 0

    lax.fori_loop(0, cols // BLOCK, order_rows, 0)

    def reorder(value, back):
        count = value.shape[0]
        pieces = []
        rest = value
        for part in range(3):
            pieces.append(rest.astype(jnp.bfloat16))
            if part < 2:
                rest = rest - pieces[-1].astype(jnp.float32)
        got = lax.dot_general(
            jnp.concatenate(pieces, axis=0), order[...], (((1,), (1 if back else 0,)), ((), ())),
            preferred_element_type=jnp.float32,
        )
        return got[:count] + got[count : 2 * count] + got[2 * count :]

    def each_block(body):
        def step(i, _):
            body(pl.multiple_of(i * BLOCK, BLOCK))
            return 0

        lax.fori_loop(0, rows // BLOCK, step, 0)

    def enter(src, buf):
        def body(r):
            got = reorder(src[pl.ds(r, BLOCK), :], False)
            here = pl.ds(pl.multiple_of(HALO + r, 8), BLOCK)
            for c in range(tiles):
                buf[c, here, :] = got[:, c * LANES : (c + 1) * LANES]

        each_block(body)

    def leave(buf, dst):
        def body(r):
            here = pl.ds(pl.multiple_of(HALO + r, 8), BLOCK)
            whole = jnp.concatenate([buf[c, here, :] for c in range(tiles)], axis=1)
            dst[pl.ds(r, BLOCK), :] = reorder(whole, True)

        each_block(body)

    def in_place(ref):
        def body(r):
            ref[pl.ds(r, BLOCK), :] = reorder(ref[pl.ds(r, BLOCK), :], False)

        each_block(body)

    def pack(buf, slot, first, count):
        lane = lanes_of(8 * count)
        here = slice(HALO + 8 * first, HALO + 8 * (first + count))
        there = slice(8 * first, 8 * (first + count))
        tile = [buf[c, here, :] for c in range(tiles)]
        for side in range(2):
            out = None
            for c in range(tiles):
                by = EDGE * (c + side) % LANES
                turned = pltpu.roll(tile[c], by, 1) if by else tile[c]
                out = turned if out is None else jnp.where(lane < EDGE * c, out, turned)
            packs[slot, side, there, :] = out

    def unpack(buf, slot, first, last, turns):
        unit = 8 * (last - first) // turns

        def body(i, _):
            r = pl.ds(pl.multiple_of(first * 8 + i * unit, 8), unit)
            lane = lanes_of(unit)
            near, far = strips[slot, 0, r, :], strips[slot, 1, r, :]
            for c in range(tiles):
                by, bx = (LANES - EDGE * c) % LANES, EDGE * (tiles - 1 - c)
                a = pltpu.roll(near, by, 1) if by else near
                b = pltpu.roll(far, bx, 1) if bx else far
                buf[tiles + c, r, :] = jnp.where(lane < LANES // 2, a, b)
            return 0

        lax.fori_loop(0, turns, body, 0)

    def take_end(buf, slot, side):
        start = (0, high)[side]
        for c in range(tiles):
            buf[c, start : start + HALO, :] = ends[slot, side, c]

    def exchange(buf, slot):
        index = iter(range(COPIES))

        def send(src, dst, i, j):
            at = next(index)
            return pltpu.make_async_remote_copy(
                src_ref=src,
                dst_ref=dst,
                send_sem=send_sem.at[slot, at],
                recv_sem=recv_sem.at[slot, at],
                device_id=(i, j),
                device_id_type=MESH,
            )

        def rows_to(first, count, start, i):
            return [
                send(
                    packs.at[slot, which, pl.ds(first, count), :],
                    strips.at[slot, which, pl.ds(start, count), :],
                    i, j,
                )
                for which, j in ((0, left), (1, right))
            ]

        def north(first, count):
            return [
                send(
                    buf.at[pl.ds(0, tiles), pl.ds(low + first, count), :],
                    ends.at[slot, 1, :, pl.ds(first, count), :],
                    up, y,
                )
            ] + rows_to(first, count, high + first, up)

        def south(first, count):
            start = first - (rows - HALO)
            return [
                send(
                    buf.at[pl.ds(0, tiles), pl.ds(low + first, count), :],
                    ends.at[slot, 0, :, pl.ds(start, count), :],
                    down, y,
                )
            ] + rows_to(first, count, start, down)

        def side(first, count):
            return rows_to(first, count, low + first, x)

        rest, half = HALO - CHUNK, CHUNK // 2
        end_d = [south(rows - CHUNK + part * half, half) for part in range(2)]
        side_d = [side(rows - CHUNK + part * half, half) for part in range(2)]
        end_a = [north(part * half, half) for part in range(2)]
        side_a = [side(part * half, half) for part in range(2)]
        side_c = side(2 * CHUNK - 8, CHUNK + 8)
        top_c = north(CHUNK, rest)
        late_c = side(CHUNK, 8) + south(rows - HALO, rest)
        side_b = side(HALO, CHUNK - 16)
        parts = {
            "d0": end_d[0] + side_d[0],
            "d1": end_d[1] + side_d[1],
            "a0": end_a[0] + side_a[0],
            "a1": end_a[1] + side_a[1],
            "c": side_c + top_c + late_c,
            "b": side_b,
        }
        early = end_a[0] + end_a[1] + top_c + side_d[0] + side_d[1] + side_c
        late = end_d[0] + end_d[1] + side_a[0] + side_a[1] + late_c + side_b
        return parts, early, late

    def weights_pass(n):
        def body(i, _):
            r = pl.ds(pl.multiple_of(i * 8, 8), 8)
            for c in range(tiles):
                lanes = pl.ds(c * LANES, LANES)
                wx = catmull(fr[n, 0, r, lanes])
                wy = catmull(fr[n, 1, r, lanes])
                for a in range(4):
                    for b in range(4):
                        wts[c, i, a * 4 + b] = wx[a] * wy[b]
            return 0

        lax.fori_loop(0, groups, body, 0)

    def shift(src, dst, n, k, row0, sign):
        a, b = sign * off[n, 0, k], sign * off[n, 1, k]
        start = HALO + row0 + a - 1
        lane = lanes_of(PIECE)
        held = {}

        def turn(m, p, first, second, split, amount):
            r = pl.ds(start + p, PIECE)
            both = jnp.where(lane < split, src[first, r, :], src[second, r, :])
            held[m, p] = pltpu.roll(both, amount, 1)

        def put(m, p):
            dst[k, m, p : p + PIECE, :] = held.pop((m, p))

        turns, puts = [], []
        for m in range(taps):
            total = b + (m - 1)
            tile = lax.bitwise_and(total, tiles - 1)
            by = lax.shift_right_arithmetic(total, tiles.bit_length() - 1)
            below = tiles * lax.shift_right_logical(by, 31)
            split = lax.bitwise_and(by, LANES - 1)
            amount = lax.bitwise_and(-by, LANES - 1)
            for p in range(0, GROWS, PIECE):
                turns.append(functools.partial(turn, m, p, tile + tiles - below, tile + below, split, amount))
                puts.append(functools.partial(put, m, p))
        return turns, puts

    def staggered(turns, puts, lag):
        for at in range(len(turns) + lag):
            now = []
            if at < len(turns):
                now.append(turns[at])
            if at >= lag:
                now.append(puts[at - lag])
            yield now

    def weave(main, side):
        done = 0
        for at, step in enumerate(main):
            step()
            due = (at + 1) * len(side) // len(main)
            for i in range(done, due):
                for one in side[i]:
                    one()
            done = due

    def sample(src, w, k, c, j):
        acc = None
        for a in range(4):
            for b in range(4):
                part = w[a * 4 + b] * src[k, c + b, pl.ds(j + a, 8), :]
                acc = part if acc is None else acc + part
        return acc

    def backward_rows(src, dst, n, row0, i):
        j = pl.multiple_of(i * 8, 8)
        g = row0 // 8 + i
        r = pl.ds(pl.multiple_of(row0 + j, 8), 8)
        here = pl.ds(pl.multiple_of(HALO + row0 + j, 8), 8)
        out = []
        for c in range(tiles):
            w, q = [], []

            def take(k, c=c, w=w, q=q):
                if k == 0:
                    w.extend(wts[c, g, m] for m in range(16))
                q.append(sample(src, w, k, c, j) + time_step * cost[n, k])
                if k == controls - 1:
                    lowest = functools.reduce(jnp.minimum, q)
                    edge = lowest + temper
                    total = None
                    for kk in range(controls):
                        ramp = jnp.maximum(edge - q[kk], 0.0)
                        ramps[n, c, g, kk] = ramp
                        total = ramp if total is None else total + ramp
                    recip[n, c, g] = 1.0 / total
                    dst[c, here, :] = lowest + time_step * cr[r, pl.ds(c * LANES, LANES)]

            out += [functools.partial(take, k) for k in range(controls)]
        return out

    def forward_rows(src, dst, n, row0, i):
        j = pl.multiple_of(i * 8, 8)
        g = row0 // 8 + i
        here = pl.ds(pl.multiple_of(HALO + row0 + j, 8), 8)
        out, added = [], []
        for c in range(tiles):
            w, q = [], []

            def take(k, c=c, w=w, q=q):
                if k == 0:
                    w.extend(wts[c, g, m] for m in range(16))
                q.append(sample(src, w, k, c, j))
                if k == controls - 1:
                    acc = None
                    for kk in range(controls):
                        part = ramps[n, c, g, kk] * q[kk]
                        acc = part if acc is None else acc + part
                    arrived = jnp.maximum(acc * recip[n, c, g], 0.0)
                    dst[c, here, :] = arrived
                    added.append(arrived)
                    if c == tiles - 1:
                        sums[n] = sums[n] + functools.reduce(jnp.add, added)

            out += [functools.partial(take, k) for k in range(controls)]
        return out

    per = CHUNK // 8
    mine = {"d": rows - CHUNK, "a": 0, "c": 2 * CHUNK, "b": CHUNK}

    def stage(src, dst, slot_src, slot_dst, n, sign, rows_fn, send, fresh):
        if fresh:
            in_place(fr.at[n, 0])
            in_place(fr.at[n, 1])
        weights_pass(n)
        _, early, late = exchange(src, slot_src)
        for d in early:
            d.wait()
        unpack(src, slot_src, 2 * (low // 8) + 6, (high + HALO) // 8, 2)
        take_end(src, slot_src, 1)

        def first(k, _):
            one, two = (shift(src, ga, n, 2 * k + u, mine["d"], sign) for u in range(2))
            for now in staggered(one[0] + two[0], one[1] + two[1], 20):
                for step in now:
                    step()
            return 0

        lax.fori_loop(0, controls // 2, first, 0)
        for d in late:
            d.wait()
        unpack(src, slot_src, 0, 2 * (low // 8) + 6, 3)
        take_end(src, slot_src, 0)
        parts, _, _ = exchange(dst, slot_dst)

        def put_out(name, pieces):
            for at, count in pieces:
                pack(dst, slot_dst, at, count)
            for d in parts[name]:
                d.start()

        def publish(name, pieces):
            if send is True:
                put_out(name, pieces)
            else:
                pl.when(send)(functools.partial(put_out, name, pieces))

        def block(now, later, name, following, start, stop, place, halves=False):
            def body(i, _):
                side = []
                if following is not None:
                    side = list(staggered(*shift(src, later, n, i, mine[following], sign), LAG))
                weave(rows_fn(now, dst, n, mine[name], place(i)), side)
                if halves:
                    for part in range(2):
                        ready = i == (part + 1) * per // 2 - 1
                        if send is not True:
                            ready = jnp.logical_and(ready, send)
                        at = mine[name] // 8 + part * (per // 2)

                        @pl.when(ready)
                        def _(part=part, at=at):
                            put_out(f"{name}{part}", [(at, per // 2)])

                return 0

            lax.fori_loop(start, stop, body, 0)

        def plain(i):
            return i

        block(ga, gb, "d", "a", 0, per, plain, True)
        block(gb, ga, "a", "c", 0, per, plain, True)
        block(ga, gb, "c", "b", 0, per, plain)
        block(gb, None, "b", None, 0, 2, lambda i: (per - 1) * (1 - i))
        publish("c", [(mine["c"] // 8 - 1, per + 1), (per, 1)])
        block(gb, None, "b", None, 1, per - 1, plain)
        publish("b", [(per + 1, per - 2)])

    def begin(load, src, buf, slot):
        load.wait()
        enter(src, buf)
        for part in range(4):
            pack(buf, slot, part * (groups // 4), groups // 4)
        _, early, late = exchange(buf, slot)
        return early + late

    first = begin(load_term, stage_a, ea, 0)
    pl.semaphore_wait(barrier, 8)
    for d in first:
        d.start()
    for d in begin(load_dens, stage_b, ec, 2):
        d.start()
    load_cr.wait()
    in_place(cr)
    for copy in load_fr:
        copy.wait()
    sums[...] = jnp.zeros_like(sums)

    def backward_pair(m, _):
        n = steps - 1 - 2 * m
        stage(ea, eb, 0, 1, n, 1, backward_rows, True, True)
        stage(eb, ea, 1, 0, n - 1, 1, backward_rows, m + 1 < steps // 2, True)
        return 0

    lax.fori_loop(0, steps // 2, backward_pair, 0)
    leave(ea, stage_a)
    store_value = pltpu.make_async_copy(stage_a, value_out, load_sem.at[0])
    store_value.start()

    def forward_pair(m, _):
        n = 2 * m
        stage(ec, ea, 2, 0, n, -1, forward_rows, True, False)
        stage(ea, ec, 0, 2, n + 1, -1, forward_rows, m + 1 < steps // 2, False)
        return 0

    lax.fori_loop(0, steps // 2, forward_pair, 0)

    def spread(part, count, at, own, first):
        copies = []
        for hop in range(1, count):
            copies.append(
                pltpu.make_async_remote_copy(
                    src_ref=part.at[0],
                    dst_ref=part.at[hop],
                    send_sem=sum_send.at[first + hop],
                    recv_sem=sum_recv.at[first + hop],
                    device_id=at(lax.rem(own + hop, count)),
                    device_id_type=MESH,
                )
            )
        for copy in copies:
            copy.start()

        def finish():
            for copy in copies:
                copy.wait()
            total = part[0]
            for hop in range(1, count):
                total = total + part[hop]
            return total

        return finish

    own = [jnp.sum(sums[n], axis=0, keepdims=True) for n in range(steps)]
    part_y[0] = jnp.concatenate(own + [jnp.zeros((8 - steps, LANES), jnp.float32)], axis=0)
    finish_y = spread(part_y, ny, lambda j: (x, j), y, 0)
    leave(ec, stage_b)
    store_mass = pltpu.make_async_copy(stage_b, mass_out, load_sem.at[1])
    store_mass.start()
    part_x[0] = finish_y()
    finish_x = spread(part_x, nx, lambda i: (i, y), x, ny)
    store_mass.wait()
    store_value.wait()
    whole = finish_x()
    totals = jnp.sum(whole, axis=1, keepdims=True) * (1.0 / (rows * cols * nx * ny))
    totals_out[...] = jnp.broadcast_to(totals, (8, LANES))


def finish_kernel(value, mass, totals, value_out, mass_out, masses_out):
    steps = masses_out.shape[0]
    scale = jnp.float32(1.0)
    for n in range(steps):
        mean = totals[n, 0] / scale
        masses_out[n] = mean
        scale = scale * (mean + epsilon)
    factor = 1.0 / jnp.full(mass.shape, scale, jnp.float32)
    value_out[...] = value[...]
    mass_out[...] = mass[...] * factor


def shards(terminal, crowding, density, fractions, offsets, control_cost):
    rows, cols = terminal.shape
    tiles = cols // LANES
    steps, controls = control_cost.shape
    nx, ny = lax.axis_size("gx"), lax.axis_size("gy")
    field = jax.ShapeDtypeStruct((rows, cols), jnp.float32)
    tall = rows + 2 * HALO

    def vmem(*shape):
        return pltpu.VMEM(shape, jnp.float32)

    smem = pl.BlockSpec(memory_space=pltpu.SMEM)
    hbm = pl.BlockSpec(memory_space=pl.ANY)
    value, mass, totals = pl.pallas_call(
        kernel,
        out_shape=(field, field, jax.ShapeDtypeStruct((8, LANES), jnp.float32)),
        in_specs=[smem, smem, hbm, hbm, hbm, hbm],
        out_specs=(hbm, hbm, pl.BlockSpec(memory_space=pltpu.VMEM)),
        scratch_shapes=[
            vmem(steps, 8, LANES),
            vmem(ny, 8, LANES),
            vmem(nx, 8, LANES),
            vmem(2 * tiles, tall, LANES),
            vmem(2 * tiles, tall, LANES),
            vmem(2 * tiles, tall, LANES),
            vmem(3, 2, tiles, HALO, LANES),
            vmem(3, 2, tall, LANES),
            vmem(3, 2, rows, LANES),
            vmem(controls, tiles + 3, GROWS, LANES),
            vmem(controls, tiles + 3, GROWS, LANES),
            vmem(tiles, rows // 8, 16, 8, LANES),
            vmem(steps, tiles, rows // 8, controls, 8, LANES),
            vmem(steps, tiles, rows // 8, 8, LANES),
            vmem(rows, cols),
            vmem(steps, 2, rows, cols),
            vmem(rows, cols),
            vmem(rows, cols),
            pltpu.VMEM((cols, cols), jnp.bfloat16),
            pltpu.SemaphoreType.DMA((3 + steps,)),
            pltpu.SemaphoreType.DMA((3, COPIES)),
            pltpu.SemaphoreType.DMA((3, COPIES)),
            pltpu.SemaphoreType.DMA((nx + ny,)),
            pltpu.SemaphoreType.DMA((nx + ny,)),
        ],
        compiler_params=pltpu.CompilerParams(
            collective_id=0, has_side_effects=True, vmem_limit_bytes=60 * 2**20
        ),
    )(jnp.swapaxes(offsets, 1, 2), control_cost, terminal, crowding, density, fractions)
    whole = pl.BlockSpec(memory_space=pltpu.VMEM)
    return pl.pallas_call(
        finish_kernel,
        out_shape=(field, field, jax.ShapeDtypeStruct((steps,), jnp.float32)),
        in_specs=[whole, whole, smem],
        out_specs=(whole, whole, smem),
    )(value, mass, totals)


def solution(mesh):
    placed = (P("gx", "gy"), P("gx", "gy"), P("gx", "gy"), P(None, None, "gx", "gy"), P(), P())
    return jax.shard_map(
        shards,
        mesh=mesh,
        in_specs=placed,
        out_specs=(P("gx", "gy"), P("gx", "gy"), P()),
        check_vma=False,
    )
```
